512 devices in a mesh: owner: 32 (over z, core), sub: 16 (over x, y).
Axes of the slice: x: 4, y: 4, z: 16, core: 2. Of those that a mesh axis runs over, the one named last changes fastest.
Arguments:
- residual: float32 [256, 73728], P('owner', 'sub'), may hold values from -6 to 6
- counts: int32 [32, 64], P('owner', 'sub'), may hold values from 1 to 36
- assembly: int32 [32, 64, 36, 2304], P('owner', 'sub'), may hold values from 0 to 1, as said below
- level_two: float32 [32, 2304, 2304], P('owner', 'sub'), as said below
- block_inverse: float32 [32, 2304, 144], P('owner', 'sub'), as said below
Outputs:
- corrections: float32 [256, 73728], P('owner', 'sub')
- level_residual: float32 [32, 2304, 256], P('owner', 'sub')
The draws below stay inside these ranges and needn't reach their ends.
Inputs may be any that keep to these rules, and one draw needn't show every extreme that they name: `assembly`: every row of each [36, 2304] block holds exactly one 1; split the 2304 columns into 16 equal ranges and a group's positions into runs of 4: the 144 rows of one run (live or not) put at most 18 of their 1s into one range, and in every run some range gets exactly 18. `level_two`: each group's matrix is symmetric positive definite. `block_inverse`: each diagonal block is symmetric positive definite.
All inputs are finite; a program needn't handle non-finite values.
Results may differ from the reference program's by a relative error of at most 0.0003.
Values sent between devices are 32-bit elements; how exact they have to be, the bound alone decides.
A program may use at most 64 MiB of HBM per device.

```python
import math
import jax
import jax.numpy as jnp
from jax import lax

PRIM = 36
NC = 2304
BLOCK = 144
ITERS = 4
SUB_DEV = 4
RHS = 256
GSUBS = 64
GROUPS = 32
SUBS = 2048
ROUTE = 18
N_OWNER = 32
N_SUB = 16


def one_run(key):
    rows = SUB_DEV * PRIM
    held = NC // N_SUB
    key_a, key_b, key_c, key_d = jax.random.split(key, 4)
    first = jax.random.randint(key_a, (), 0, N_SUB).astype(jnp.int32)
    others = jax.random.permutation(key_b, (N_SUB - 1) * ROUTE).astype(jnp.int32)
    other_holder = others // ROUTE
    other_holder = other_holder + (other_holder >= first).astype(jnp.int32)
    holders = jnp.concatenate([jnp.zeros((ROUTE,), jnp.int32) + first, other_holder[:rows - ROUTE]])
    holders = jax.random.permutation(key_c, holders)
    offsets = jax.random.randint(key_d, (rows,), 0, held).astype(jnp.int32)
    return holders * held + offsets


def draw_assembly(key, part):
    keys = jax.random.split(jax.random.fold_in(key, 11), GROUPS * N_SUB)
    picks = jax.vmap(one_run)(keys).reshape(GROUPS, GSUBS, PRIM)
    columns = lax.broadcasted_iota(jnp.int32, (GROUPS, GSUBS, PRIM, NC), 3)
    return (columns == picks[..., None]).astype(jnp.int32)


def one_matrix(key):
    key_a, key_b, key_c = jax.random.split(key, 3)
    noise = jax.random.normal(key_a, (NC, NC), jnp.float32)
    eye = jnp.eye(NC, dtype=jnp.float32)
    off = (noise + noise.T) * (0.5 / math.sqrt(NC)) * (1.0 - eye)
    rowsum = jnp.sum(jnp.abs(off), axis=1)
    lift = jax.random.uniform(key_b, (NC,), jnp.float32, 0.05, 1.0) * jnp.mean(rowsum)
    diag = 1.25 * rowsum + lift
    matrix = (off + diag[:, None] * eye) / jnp.mean(diag)
    return matrix


def draw_level_two(key, part):
    keys = jax.random.split(jax.random.fold_in(key, 23), GROUPS)
    return lax.map(one_matrix, keys)


def draw_block_inverse(key, part):
    nblocks = NC // BLOCK
    key_a, key_b = jax.random.split(jax.random.fold_in(key, 37))
    noise = jax.random.uniform(key_a, (GROUPS, nblocks, BLOCK, BLOCK), jnp.float32, -1.0, 1.0)
    eye = jnp.eye(BLOCK, dtype=jnp.float32)
    off = (noise + jnp.swapaxes(noise, 2, 3)) * (0.2 / BLOCK) * (1.0 - eye)
    diag = jnp.exp(jax.random.uniform(key_b, (GROUPS, nblocks, BLOCK), jnp.float32, -0.7, 0.7))
    blocks = off + diag[..., None] * eye
    return blocks.reshape(GROUPS, NC, BLOCK)


def with_ends(values, key, low, largest):
    extent = values.shape
    spot = [jax.random.randint(jax.random.fold_in(key, axis), (), 0, extent[axis]) for axis in range(len(extent))]
    values = values.at[tuple(spot)].set(low)
    longest = extent.index(max(extent))
    spot[longest] = (spot[longest] + 1) % extent[longest]
    return values.at[tuple(spot)].set(largest)


def block_scale(own_key, extent, cuts, smallest, largest):
    gain, own = 1.0, jax.random.fold_in(own_key, 6)
    for position, shards_of in cuts:
        steps = jnp.exp(jax.random.uniform(jax.random.fold_in(own, position), (shards_of,), jnp.float32, smallest / len(cuts), largest / len(cuts)))
        gain = gain * jnp.repeat(steps, extent[position] // shards_of).reshape([-1 if axis == position else 1 for axis in range(len(extent))])
    return gain


def gaussian(own_key, shape, width, most, shards=(), kind=jnp.bfloat16):
    array = width * jax.random.normal(own_key, shape, jnp.float32)
    if shards:
        array = array * block_scale(own_key, shape, shards, -0.22, 0.18)
    return jnp.clip(array, -most, most).astype(kind)


def setup_inputs(seed: int = 0) -> dict:
    key_list = jax.random.split(jax.random.key(seed), 6)
    return {
        "residual": gaussian(key_list[0], (RHS, SUBS * PRIM), 1.0, 6.0, ((0, 32), (1, 16)), jnp.float32),
        "counts": with_ends(jax.random.randint(key_list[1], (GROUPS, GSUBS), 1, PRIM + 1), jax.random.fold_in(key_list[1], 1), 1, PRIM).astype(jnp.int32),
        "assembly": draw_assembly(jax.random.fold_in(key_list[5], 71), 0),
        "level_two": draw_level_two(jax.random.fold_in(key_list[5], 71), 0),
        "block_inverse": draw_block_inverse(jax.random.fold_in(key_list[5], 71), 0),
    }


def precondition(inverse, vector):
    nblocks = NC // BLOCK
    blocks = inverse.reshape(nblocks, BLOCK, BLOCK)
    shaped = vector.reshape(nblocks, BLOCK, RHS)
    return jnp.einsum("bij,bjr->bir", blocks, shaped, precision=lax.Precision.HIGHEST).reshape(NC, RHS)


def solve_group(items):
    local, count_row, blocks, matrix, inverse = items
    live = (lax.broadcasted_iota(jnp.int32, (GSUBS, PRIM), 1) < count_row[:, None]).astype(jnp.float32)
    basis = blocks.reshape(GSUBS * PRIM, NC).astype(jnp.float32) * live.reshape(GSUBS * PRIM)[:, None]
    rhs = jnp.dot(basis.T, local, precision=lax.Precision.HIGHEST, preferred_element_type=jnp.float32)
    solution = jnp.zeros((NC, RHS), jnp.float32)
    resid = rhs
    zvec = precondition(inverse, resid)
    direction = zvec
    rz_now = jnp.sum(resid * zvec, axis=0)
    for step in range(ITERS):
        image = jnp.dot(matrix, direction, precision=lax.Precision.HIGHEST, preferred_element_type=jnp.float32)
        alpha = rz_now / jnp.sum(direction * image, axis=0)
        solution = solution + alpha * direction
        resid = resid - alpha * image
        zvec = precondition(inverse, resid)
        rz_next = jnp.sum(resid * zvec, axis=0)
        direction = zvec + (rz_next / rz_now) * direction
        rz_now = rz_next
    corr = jnp.dot(basis, solution, precision=lax.Precision.HIGHEST, preferred_element_type=jnp.float32)
    return corr, resid


def reference(residual, counts, assembly, level_two, block_inverse):
    shaped = residual.reshape(RHS, N_SUB, N_OWNER, SUB_DEV, PRIM)
    local = jnp.transpose(shaped, (2, 1, 3, 4, 0)).reshape(N_OWNER, GSUBS * PRIM, RHS)
    corr, resid = lax.map(solve_group, (local, counts, assembly, level_two, block_inverse))
    back = corr.reshape(N_OWNER, N_SUB, SUB_DEV, PRIM, RHS)
    corrections = jnp.transpose(back, (4, 1, 0, 2, 3)).reshape(RHS, SUBS * PRIM)
    return corrections, resid
```

```python
import functools

import jax
import jax.numpy as jnp
from jax import lax
from jax.experimental import pallas as pl
from jax.experimental.pallas import tpu as pltpu
from jax.sharding import PartitionSpec as P

ITERS = 4
F32 = jnp.float32
BF16 = jnp.bfloat16
OWN = 32
SUB = 16
SIDE = 4
BLK = 144
SLOT = 18
PRIM = 36
LANES = 128
HALF = 64
PACK = 2 * BLK
MSG = 40
VEC = PACK + 8
CUT = 152


def iota(shape, dim):
    return lax.broadcasted_iota(jnp.int32, shape, dim)


def dot(a, b):
    return jnp.dot(a, b, preferred_element_type=F32)


def dot_nt(a, b):
    return lax.dot_general(a, b, (((1,), (1,)), ((), ())), preferred_element_type=F32)


def dot_tn(a, b):
    return lax.dot_general(a, b, (((0,), (0,)), ((), ())), preferred_element_type=F32)


def split(x):
    hi = x.astype(BF16)
    return hi, (x - hi.astype(F32)).astype(BF16)


def half_swap(x):
    return pltpu.roll(x, HALF, 1)


def low_half(shape):
    return iota(shape, 1) < HALF


def block_transpose(t):
    away = iota((8, LANES), 0) - iota((8, LANES), 1) // 16
    out = t
    for shift in range(1, 8):
        moved = pltpu.roll(pltpu.roll(t, shift, 0), LANES - 16 * shift, 1)
        out = jnp.where((away & 7) == shift, moved, out)
    return out


def kernel(
    res_ref, cnt_ref, asm_ref, mat_ref, inv_ref,
    corr_ref, resid_ref,
    zmain, ztail, zmain_in, ztail_in,
    cmain, ctail, cmain_in, ctail_in,
    offs, offs_in, info,
    rows_in, inv_in, stack, mstack,
    vsend, vin, land, land_t, pick,
    gsend, gin, wide, ssend, sin,
    psend, pin, back, rbuf, rin, local,
    zs_m, zr_m, zs_t, zr_t, cs_m, cr_m, cs_t, cr_t,
    os, orr, ms, mr, ivs, ivr, vs, vr, gs, gr, ss, sr, ps, pr, rs, rr,
):
    owner = lax.axis_index("owner")
    sub = lax.axis_index("sub")
    core = lax.rem(owner, 2)
    sx, sy = sub // SIDE, lax.rem(sub, SIDE)
    a = sx * (1 - core) + sy * core
    c = sy * (1 - core) + sx * core

    def at(ra, rc):
        return (4 * ra + rc) * (1 - core) + (4 * rc + ra) * core

    def ring(v, step):
        return lax.rem(v + step + SIDE, SIDE)

    def rcopy(src, dst, ssem, rsem, dev):
        return pltpu.make_async_remote_copy(
            src_ref=src, dst_ref=dst, send_sem=ssem, recv_sem=rsem,
            device_id=dev, device_id_type=pl.DeviceIdType.MESH,
        )

    barrier = pltpu.get_barrier_semaphore()

    @pl.loop(1, OWN)
    def _(j):
        pl.semaphore_signal(barrier, inc=1, device_id=(lax.rem(owner + j, OWN), sub),
                            device_id_type=pl.DeviceIdType.MESH)

    @pl.loop(1, SUB)
    def _(j):
        pl.semaphore_signal(barrier, inc=1, device_id=(owner, lax.rem(sub + j, SUB)),
                            device_id_type=pl.DeviceIdType.MESH)

    lane = iota((8, LANES), 1)
    low = low_half((8, LANES))

    def tile(t):
        return res_ref[:, LANES * t:LANES * (t + 1)]

    for k in range(4):
        tails = None
        for j in range(8):
            g = 8 * k + j
            if j == 0:
                main = tile(g + k)
            else:
                main = pltpu.roll(
                    jnp.where(lane >= 16 * j, tile(g + k), tile(g + k + 1)), LANES - 16 * j, 1
                )
            zmain[g] = main
            nxt = tile(g + k + 1)
            tails = nxt if j == 0 else jnp.where(lane // 16 == j, nxt, tails)
        moved = block_transpose(tails)
        for j in range(8):
            ztail[8 * k + j] = moved[j:j + 1, :]

    col = iota((8, SUB * BLK), 1)
    holder_of = col // BLK
    which = jnp.where(iota((8, SUB * BLK), 0) == 0, col - holder_of * BLK, holder_of)
    which = which.astype(F32).astype(BF16)
    info[...] = jnp.zeros_like(info)
    for j in range(4):
        block = asm_ref[j].astype(F32).astype(BF16)
        info[:, PRIM * j:PRIM * (j + 1)] = dot_nt(which, block)
    place8 = info[...]
    inside = place8.astype(BF16)
    held = place8[1:2, :].astype(jnp.int32)
    dof = iota((1, 256), 1)
    which_sub = ((dof >= PRIM).astype(jnp.int32) + (dof >= 2 * PRIM).astype(jnp.int32)
                 + (dof >= 3 * PRIM).astype(jnp.int32))
    count = jnp.where(which_sub == 0, cnt_ref[0, 0], jnp.where(
        which_sub == 1, cnt_ref[0, 1], jnp.where(which_sub == 2, cnt_ref[0, 2], cnt_ref[0, 3])))
    live = ((dof - PRIM * which_sub) < count) & (dof < BLK)
    held = jnp.where(live, held, -1)
    hot = (held == iota((SUB, 256), 0)).astype(F32)
    upper = (iota((256, 256), 0) < iota((256, 256), 1)).astype(F32).astype(BF16)
    rank = jnp.sum(hot * dot(hot.astype(BF16), upper), axis=0, keepdims=True).astype(jnp.int32)
    hx, hy = held // SIDE, held & 3
    ha = hx * (1 - core) + hy * core
    hk = hy * (1 - core) + hx * core
    spot = ha * LANES + (hk // 2) * HALF + (hk & 1) * SLOT + rank
    spot = jnp.where(live, spot, -1)
    pick[...] = (iota((4 * LANES, 256), 0) == spot).astype(F32).astype(BF16)
    rows = dot_nt(inside, pick[...])
    for j in range(4):
        offs[j] = rows[0:1, LANES * j:LANES * (j + 1)]

    pl.semaphore_wait(barrier, OWN - 1 + SUB - 1)

    @pl.loop(1, OWN)
    def _(j):
        peer = lax.rem(owner + j, OWN)
        rcopy(zmain.at[peer], zmain_in.at[owner], zs_m.at[peer], zr_m.at[owner], (peer, sub)).start()
        rcopy(ztail.at[peer], ztail_in.at[owner], zs_t.at[peer], zr_t.at[owner], (peer, sub)).start()

    def off_copy(peer, pa):
        return rcopy(offs.at[pa], offs_in.at[sub], os.at[peer], orr.at[sub], (owner, peer))

    def group_of(peer):
        px, py = peer // SIDE, lax.rem(peer, SIDE)
        return px * (1 - core) + py * core, py * (1 - core) + px * core

    @pl.loop(1, SUB)
    def _(j):
        peer = lax.rem(sub + j, SUB)
        pa, _pc = group_of(peer)
        off_copy(peer, pa).start()

    nextc, prevc = ring(c, 1), ring(c, -1)
    oppc = ring(c, 2)
    c_right, c_left, c_opp = (owner, at(a, nextc)), (owner, at(a, prevc)), (owner, at(a, oppc))
    for n, dev in ((0, c_right), (1, c_left), (2, c_opp)):
        rcopy(inv_ref, inv_in.at[c], ivs.at[n], ivr.at[n], dev).start()

    top, bottom = pl.ds(0, BLK // 2), pl.ds(BLK // 2, BLK // 2)

    def mat_copy(n, slot, part, dev, src=None):
        source = mat_ref.at[part] if src is None else src
        return rcopy(source, rows_in.at[slot, part], ms.at[n], mr.at[n], dev)

    mat_copy(0, c, top, c_right).start()
    mat_copy(2, c, bottom, c_left).start()
    mat_copy(1, c, bottom, c_right).start()
    mat_copy(3, c, top, c_left).start()

    zmain_in[owner] = zmain[owner]
    ztail_in[owner] = ztail[owner]
    offs_in[sub] = offs[a]
    inv_in[c] = inv_ref[...]
    vin[:, MSG:HALF, :] = jnp.zeros((SUB, HALF - MSG, LANES), F32)
    back[...] = jnp.zeros_like(back)

    @pl.loop(1, SUB)
    def _(j):
        peer = lax.rem(sub + j, SUB)
        rcopy(offs.at[0], offs_in.at[peer], os.at[peer], orr.at[peer], (owner, peer)).wait_recv()

    lane1 = iota((1, LANES), 1)
    extra = jnp.where((lane1 & (HALF - 1)) >= SLOT, float(BLK), 0.0)
    for m in range(SUB // 2):
        one, two = offs_in[2 * m], offs_in[2 * m + 1]
        for h in range(2):
            if h == 0:
                row = jnp.where(lane1 < HALF, one, half_swap(two)) + extra
            else:
                row = jnp.where(lane1 < HALF, half_swap(one), two) + extra
            rowi = row.astype(jnp.int32)
            cols = pl.ds(LANES * m, LANES)
            land[h, :, cols] = (iota((PACK, LANES), 0) == rowi).astype(F32).astype(BF16)
            down = jnp.broadcast_to(row, (LANES, LANES)).T.astype(jnp.int32)
            for t, width in ((0, LANES), (1, LANES), (2, PACK - 2 * LANES)):
                hit = (down == iota((LANES, LANES), 1) + LANES * t).astype(F32).astype(BF16)
                land_t[h, cols, LANES * t:LANES * t + width] = hit[:, :width]

    def store_rows(slot, x):
        hi, lo = split(x)
        at_hi = pl.multiple_of(slot * BLK, 16)
        at_lo = pl.multiple_of((SIDE + slot) * BLK, 16)
        stack[pl.ds(at_hi, BLK), :] = hi
        stack[pl.ds(at_lo, BLK), :] = lo

    mat_copy(0, prevc, top, c_left).wait_recv()
    mat_copy(4, prevc, top, c_right, rows_in.at[prevc, top]).start()
    mat_copy(2, nextc, bottom, c_right).wait_recv()
    mat_copy(5, nextc, bottom, c_left, rows_in.at[nextc, bottom]).start()

    @pl.loop(1, OWN)
    def _(j):
        peer = lax.rem(owner + j, OWN)
        rcopy(zmain.at[peer], zmain_in.at[peer], zs_m.at[peer], zr_m.at[peer], (peer, sub)).wait_recv()
        rcopy(ztail.at[peer], ztail_in.at[peer], zs_t.at[peer], zr_t.at[peer], (peer, sub)).wait_recv()

    local[:, 0:LANES] = zmain_in[...].reshape(8 * OWN, LANES)
    for k in range(4):
        moved = block_transpose(ztail_in[8 * k:8 * (k + 1)].reshape(8, LANES))
        for j in range(8):
            src = 8 * k + j
            local[8 * src:8 * (src + 1), LANES:] = moved if j == 0 else pltpu.roll(
                moved, LANES - 16 * j, 1)
    loc_hi, loc_lo = split(local[...])
    vals = dot_nt(pick[...], loc_hi) + dot_nt(pick[...], loc_lo)
    low_msg = low_half((MSG, LANES))
    for ra in range(4):
        for t in range(2):
            first = vals[LANES * ra:LANES * ra + MSG, LANES * t:LANES * (t + 1)]
            second = vals[LANES * ra + HALF:LANES * ra + HALF + MSG, LANES * t:LANES * (t + 1)]
            vsend[4 * ra + 2 * t] = jnp.where(low_msg, first, half_swap(second))
            vsend[4 * ra + 2 * t + 1] = jnp.where(low_msg, half_swap(first), second)
    body = pl.ds(0, MSG)

    @pl.loop(1, SUB)
    def _(j):
        peer = lax.rem(sub + j, SUB)
        pa, pc = group_of(peer)
        rcopy(vsend.at[4 * pa + pc], vin.at[sub, body], vs.at[peer], vr.at[sub], (owner, peer)).start()

    vin[sub, body] = vsend[4 * a + c]
    store_rows(c, mat_ref[...])

    for n, slot in ((0, prevc), (1, nextc), (2, oppc)):
        rcopy(inv_ref, inv_in.at[slot], ivs.at[n], ivr.at[n], c_right).wait_recv()
    for k in range(4):
        hi, lo = split(inv_in[k])
        where_to = 2 * (k // 2) * BLK
        mstack[k % 2, where_to:where_to + BLK, :] = hi
        mstack[k % 2, where_to + BLK:where_to + 2 * BLK, :] = lo

    @pl.loop(1, SUB)
    def _(j):
        peer = lax.rem(sub + j, SUB)
        rcopy(vsend.at[0], vin.at[peer, body], vs.at[peer], vr.at[peer], (owner, peer)).wait_recv()

    low_pack = low_half((PACK, LANES))
    low_blk = low_half((BLK, LANES))

    def side_by_side(x):
        hi, lo = split(x)
        return jnp.concatenate([hi, lo], axis=1)

    def fold(x):
        return x[:, :LANES] + x[:, LANES:]

    values = side_by_side(vin[...].reshape(SUB * HALF, LANES))
    r = jnp.where(low_pack, fold(dot(land[0], values)), fold(dot(land[1], values)))

    def precond(v):
        out = []
        for kk in range(2):
            got = dot(mstack[kk], side_by_side(v[kk * BLK:(kk + 1) * BLK]))
            got = fold(got)
            out.append(jnp.where(low_blk, got[:BLK] + got[BLK:2 * BLK],
                                 got[2 * BLK:3 * BLK] + got[3 * BLK:]))
        return jnp.concatenate(out, axis=0)

    nexta, preva, oppa = ring(a, 1), ring(a, -1), ring(a, 2)
    a_right, a_left, a_opp = (owner, at(nexta, c)), (owner, at(preva, c)), (owner, at(oppa, c))
    head, rest = pl.ds(0, CUT), pl.ds(CUT, VEC - CUT)

    def vec_copy(it, n, slot, part, dev, forward=False):
        source = gin.at[it, slot, part] if forward else gsend.at[it, part]
        return rcopy(source, gin.at[it, slot, part], gs.at[it, n], gr.at[it, n], dev)

    def widen(ra, x):
        hi = x.astype(BF16).astype(F32)
        lo = x - hi
        first = jnp.where(low_pack, hi, half_swap(lo)).astype(BF16)
        second = jnp.where(low_pack, half_swap(hi), lo).astype(BF16)
        for k in range(4):
            piece = (first if k < 2 else second)[(k % 2) * BLK:(k % 2 + 1) * BLK]
            wide[pl.ds(pl.multiple_of(at(ra, k) * BLK, 16), BLK), :] = piece

    def gather_start(it, v, sums):
        gsend[it, 0:PACK] = v
        gsend[it, PACK:VEC] = sums
        vec_copy(it, 0, a, head, a_right).start()
        vec_copy(it, 2, a, rest, a_left).start()
        vec_copy(it, 1, a, rest, a_right).start()
        vec_copy(it, 3, a, head, a_left).start()
        widen(a, v)

    def gather_pass(it):
        vec_copy(it, 0, preva, head, a_left).wait_recv()
        vec_copy(it, 4, preva, head, a_right, True).start()
        vec_copy(it, 2, nexta, rest, a_right).wait_recv()
        vec_copy(it, 5, nexta, rest, a_left, True).start()
        vec_copy(it, 1, preva, rest, a_left).wait_recv()
        widen(preva, gin[it, preva, 0:PACK])
        vec_copy(it, 3, nexta, head, a_right).wait_recv()
        widen(nexta, gin[it, nexta, 0:PACK])

    def gather_end(it, sums):
        vec_copy(it, 4, oppa, head, a_right).wait_recv()
        vec_copy(it, 5, oppa, rest, a_left).wait_recv()
        widen(oppa, gin[it, oppa, 0:PACK])
        total = sums
        for ra in (preva, nexta, oppa):
            total = total + gin[it, ra, PACK:VEC]
        return total

    def product():
        got = dot(stack[...], wide[...])
        got = got[:SIDE * BLK] + got[SIDE * BLK:]
        got = got + half_swap(got)
        return jnp.where(low_pack, got[:PACK], got[PACK:])

    def column_sum(x, y):
        s = jnp.sum(x * y, axis=0, keepdims=True)
        return s + half_swap(s)

    row8 = iota((8, LANES), 0)

    def partial_sums(r, u, w):
        one, two = column_sum(r, u), column_sum(w, u)
        return jnp.where(row8 == 0, one, jnp.where(row8 == 1, two, 0.0))

    u = precond(r)
    nothing = jnp.zeros((8, LANES), F32)
    gather_start(0, u, nothing)
    gather_pass(0)

    mat_copy(1, prevc, bottom, c_left).wait_recv()
    store_rows(prevc, rows_in[prevc])
    mat_copy(3, nextc, top, c_right).wait_recv()
    store_rows(nextc, rows_in[nextc])
    mat_copy(4, oppc, top, c_right).wait_recv()
    mat_copy(5, oppc, bottom, c_left).wait_recv()
    store_rows(oppc, rows_in[oppc])

    gather_end(0, nothing)
    w = product()

    gamma = alpha = None
    x = p = s = q = z = None
    for it in range(1, ITERS):
        sums = partial_sums(r, u, w)
        m = precond(w)
        gather_start(it, m, sums)
        gather_pass(it)
        total = gather_end(it, sums)
        n = product()
        gamma_new, delta = total[0:1], total[1:2]
        if it == 1:
            alpha = gamma_new / delta
            z, q, s, p = n, m, w, u
            x = alpha * p
        else:
            beta = gamma_new / gamma
            alpha = gamma_new / (delta - beta * gamma_new / alpha)
            z, q, s, p = n + beta * z, m + beta * q, w + beta * s, u + beta * p
            x = x + alpha * p
        gamma = gamma_new
        r = r - alpha * s
        u = u - alpha * q
        w = w - alpha * z

    sums = partial_sums(r, u, w)
    ssend[...] = sums
    for n_, dev in ((0, a_right), (1, a_left), (2, a_opp)):
        rcopy(ssend, sin.at[n_], ss.at[n_], sr.at[n_], dev).start()
    total = sums
    for n_ in range(3):
        rcopy(ssend, sin.at[n_], ss.at[n_], sr.at[n_], a_right).wait_recv()
        total = total + sin[n_]
    gamma_new, delta = total[0:1], total[1:2]
    beta = gamma_new / gamma
    alpha = gamma_new / (delta - beta * gamma_new / alpha)
    s, p = w + beta * s, u + beta * p
    x = x + alpha * p
    r = r - alpha * s

    xs = side_by_side(x)
    low_slots = low_half((SUB * HALF, LANES))
    reply = jnp.where(low_slots, fold(dot(land_t[0], xs)), fold(dot(land_t[1], xs)))
    psend[...] = reply.reshape(SUB, HALF, LANES)
    mine = 4 * a + c

    @pl.loop(1, SUB)
    def _(j):
        peer = lax.rem(sub + j, SUB)
        rcopy(psend.at[peer, body], pin.at[mine], ps.at[peer], pr.at[mine], (owner, peer)).start()

    pin[mine] = psend[sub, body]

    rbuf[...] = r
    for n_, slot, dev in ((0, nextc, c_right), (1, prevc, c_left), (2, oppc, c_opp)):
        source = rbuf.at[pl.ds(pl.multiple_of(lax.rem(slot, 2) * BLK, 8), BLK)]
        rcopy(source, rin.at[c], rs.at[n_], rr.at[n_], dev).start()
    rin[c] = rbuf[pl.ds(pl.multiple_of(lax.rem(c, 2) * BLK, 8), BLK)]

    @pl.loop(1, SUB)
    def _(j):
        peer = lax.rem(sub + j, SUB)
        pa, pc = group_of(peer)
        slot = 4 * pa + pc
        rcopy(psend.at[peer, body], pin.at[slot], ps.at[peer], pr.at[slot], (owner, peer)).wait_recv()

    for ra in range(4):
        for t in range(2):
            one, two = pin[4 * ra + 2 * t], pin[4 * ra + 2 * t + 1]
            cols = slice(LANES * t, LANES * (t + 1))
            back[LANES * ra:LANES * ra + MSG, cols] = jnp.where(low_msg, one, half_swap(two))
            back[LANES * ra + HALF:LANES * ra + HALF + MSG, cols] = jnp.where(
                low_msg, half_swap(one), two)
    back_hi, back_lo = split(back[...])
    mine_back = dot_tn(back_hi, pick[...]) + dot_tn(back_lo, pick[...])
    cmain[...] = mine_back[:, :LANES].reshape(OWN, 8, LANES)
    for k in range(4):
        tails = None
        for j in range(8):
            src = 8 * k + j
            piece = mine_back[8 * src:8 * (src + 1), LANES:]
            tails = piece if j == 0 else tails + pltpu.roll(piece, 16 * j, 1)
        moved = block_transpose(tails)
        for j in range(8):
            ctail[8 * k + j] = moved[j:j + 1, :]

    @pl.loop(1, OWN)
    def _(j):
        peer = lax.rem(owner + j, OWN)
        rcopy(cmain.at[peer], cmain_in.at[owner], cs_m.at[peer], cr_m.at[owner], (peer, sub)).start()
        rcopy(ctail.at[peer], ctail_in.at[owner], cs_t.at[peer], cr_t.at[owner], (peer, sub)).start()

    cmain_in[owner] = cmain[owner]
    ctail_in[owner] = ctail[owner]

    for n_, slot in ((0, prevc), (1, nextc), (2, oppc)):
        rcopy(rbuf.at[pl.ds(0, BLK)], rin.at[slot], rs.at[n_], rr.at[n_], c_right).wait_recv()
    for t in range(2):
        one, two = rin[2 * t], rin[2 * t + 1]
        upper_half = jnp.where(low_blk, half_swap(one), two)
        lower_half = jnp.where(low_blk, one, half_swap(two))
        resid_ref[:, LANES * t:LANES * (t + 1)] = jnp.where(c < 2, lower_half, upper_half)

    for n_ in range(6):
        mat_copy(n_, c, top, c_right).wait_send()
        for it in range(ITERS):
            part = head if n_ in (0, 3, 4) else rest
            vec_copy(it, n_, a, part, a_right).wait_send()
    for n_ in range(3):
        rcopy(inv_ref, inv_in.at[c], ivs.at[n_], ivr.at[n_], c_right).wait_send()
        rcopy(ssend, sin.at[n_], ss.at[n_], sr.at[n_], a_right).wait_send()
        rcopy(rbuf.at[pl.ds(0, BLK)], rin.at[c], rs.at[n_], rr.at[n_], c_right).wait_send()

    @pl.loop(1, SUB)
    def _(j):
        peer = lax.rem(sub + j, SUB)
        rcopy(offs.at[0], offs_in.at[peer], os.at[peer], orr.at[peer], (owner, peer)).wait_send()
        rcopy(vsend.at[0], vin.at[peer, body], vs.at[peer], vr.at[peer], (owner, peer)).wait_send()
        rcopy(psend.at[peer, body], pin.at[peer], ps.at[peer], pr.at[peer], (owner, peer)).wait_send()

    @pl.loop(1, OWN)
    def _(j):
        peer = lax.rem(owner + j, OWN)
        rcopy(zmain.at[peer], zmain_in.at[peer], zs_m.at[peer], zr_m.at[peer], (peer, sub)).wait_send()
        rcopy(ztail.at[peer], ztail_in.at[peer], zs_t.at[peer], zr_t.at[peer], (peer, sub)).wait_send()
        rcopy(cmain.at[peer], cmain_in.at[peer], cs_m.at[peer], cr_m.at[peer], (peer, sub)).wait_recv()
        rcopy(ctail.at[peer], ctail_in.at[peer], cs_t.at[peer], cr_t.at[peer], (peer, sub)).wait_recv()

    @pl.loop(1, OWN)
    def _(j):
        peer = lax.rem(owner + j, OWN)
        rcopy(cmain.at[peer], cmain_in.at[peer], cs_m.at[peer], cr_m.at[peer], (peer, sub)).wait_send()
        rcopy(ctail.at[peer], ctail_in.at[peer], cs_t.at[peer], cr_t.at[peer], (peer, sub)).wait_send()

    for k in range(4):
        tails = block_transpose(ctail_in[8 * k:8 * (k + 1)].reshape(8, LANES))
        turned = [
            cmain_in[8 * k + j] if j == 0 else pltpu.roll(cmain_in[8 * k + j], 16 * j, 1)
            for j in range(8)
        ]
        for m in range(9):
            if m == 0:
                value = turned[0]
            else:
                value = jnp.where(lane < 16 * m, tails, turned[m]) if m < 8 else tails
                value = jnp.where(lane < 16 * (m - 1), turned[m - 1], value)
            where_to = LANES * (9 * k + m)
            corr_ref[:, where_to:where_to + LANES] = value


def shards(residual, counts, assembly, level_two, block_inverse):
    vmem = pl.BlockSpec(memory_space=pltpu.VMEM)
    smem = pl.BlockSpec(memory_space=pltpu.SMEM)
    anywhere = pl.BlockSpec(memory_space=pl.ANY)
    V = pltpu.VMEM
    dma = pltpu.SemaphoreType.DMA
    scratch = [
        V((OWN, 8, LANES), F32), V((OWN, 1, LANES), F32),
        V((OWN, 8, LANES), F32), V((OWN, 1, LANES), F32),
        V((OWN, 8, LANES), F32), V((OWN, 1, LANES), F32),
        V((OWN, 8, LANES), F32), V((OWN, 1, LANES), F32),
        V((SIDE, 1, LANES), F32), V((SUB, 1, LANES), F32), V((8, 256), F32),
        V((SIDE, BLK, SUB * BLK), F32), V((SIDE, BLK, BLK), F32),
        V((2 * SIDE * BLK, SUB * BLK), BF16), V((2, SIDE * BLK, BLK), BF16),
        V((SUB, MSG, LANES), F32), V((SUB, HALF, LANES), F32),
        V((2, PACK, SUB * HALF), BF16), V((2, SUB * HALF, PACK), BF16), V((4 * LANES, 256), BF16),
        V((ITERS, VEC, LANES), F32), V((ITERS, SIDE, VEC, LANES), F32),
        V((SUB * BLK, LANES), BF16), V((8, LANES), F32), V((3, 8, LANES), F32),
        V((SUB, HALF, LANES), F32), V((SUB, MSG, LANES), F32), V((4 * LANES, 256), F32),
        V((PACK, LANES), F32), V((SIDE, BLK, LANES), F32), V((256, 256), F32),
        dma((OWN,)), dma((OWN,)), dma((OWN,)), dma((OWN,)),
        dma((OWN,)), dma((OWN,)), dma((OWN,)), dma((OWN,)),
        dma((SUB,)), dma((SUB,)), dma((6,)), dma((6,)), dma((3,)), dma((3,)),
        dma((SUB,)), dma((SUB,)), dma((ITERS, 6)), dma((ITERS, 6)), dma((3,)), dma((3,)),
        dma((SUB,)), dma((SUB,)), dma((3,)), dma((3,)),
    ]
    corr, resid = pl.pallas_call(
        kernel,
        out_shape=(
            jax.ShapeDtypeStruct(residual.shape, F32),
            jax.ShapeDtypeStruct((BLK, 8 * OWN), F32),
        ),
        in_specs=[vmem, smem, vmem, vmem, vmem],
        out_specs=(vmem, vmem),
        scratch_shapes=scratch,
        compiler_params=pltpu.CompilerParams(
            collective_id=0, has_side_effects=True, vmem_limit_bytes=56 * 1024 * 1024
        ),
    )(residual, counts, assembly[0], level_two[0], block_inverse[0])
    return corr, resid[None]


def solution(mesh):
    in_specs = (
        P("owner", "sub"),
        P("owner", "sub"),
        P("owner", "sub", None, None),
        P("owner", "sub", None),
        P("owner", "sub", None),
    )
    out_specs = (P("owner", "sub"), P("owner", "sub", None))
    return jax.shard_map(shards, mesh=mesh, in_specs=in_specs, out_specs=out_specs, check_vma=False)
```

```python
import functools

import jax
import jax.numpy as jnp
from jax import lax
from jax.experimental import pallas as pl
from jax.experimental.pallas import tpu as pltpu
from jax.sharding import PartitionSpec as P

ITERS = 4
F32 = jnp.float32
BF16 = jnp.bfloat16
OWN = 32
SUB = 16
SIDE = 4
BLK = 144
SLOT = 18
PRIM = 36
LANES = 128
HALF = 64
PACK = 2 * BLK
MSG = 40
VEC = PACK + 8
TAIL = 24
CUT = 152


def iota(shape, dim):
    return lax.broadcasted_iota(jnp.int32, shape, dim)


def dot(a, b):
    return jnp.dot(a, b, preferred_element_type=F32)


def dot_nt(a, b):
    return lax.dot_general(a, b, (((1,), (1,)), ((), ())), preferred_element_type=F32)


def dot_tn(a, b):
    return lax.dot_general(a, b, (((0,), (0,)), ((), ())), preferred_element_type=F32)


def split(x):
    hi = x.astype(BF16)
    return hi, (x - hi.astype(F32)).astype(BF16)


def half_swap(x):
    return pltpu.roll(x, HALF, 1)


def low_half(shape):
    return iota(shape, 1) < HALF


def block_transpose(t):
    away = iota((8, LANES), 0) - iota((8, LANES), 1) // 16
    out = t
    for shift in range(1, 8):
        moved = pltpu.roll(pltpu.roll(t, shift, 0), LANES - 16 * shift, 1)
        out = jnp.where((away & 7) == shift, moved, out)
    return out


def kernel(
    cnt_ref, res_hbm, asm_hbm, mat_hbm, inv_hbm,
    corr_ref, resid_ref,
    res_ref, asm_ref, inv_ref, inv_out,
    zmain, ztail, zmain_in, ztail_in,
    cmain, ctail, cmain_in, ctail_in,
    offs, offs_in, info,
    rows_in, inv_in, inv_full, stack, mstack,
    vsend, vin, land, land_t, pick,
    gsend, gin, wide, ssend, sin,
    psend, pin, back, rbuf, rin, local, partial,
    loads,
    zs_m, zr_m, zs_t, zr_t, cs_m, cr_m, cs_t, cr_t,
    os, orr, ms, mr, ivs, ivr, vs, vr, gs, gr, ss, sr, ps, pr, rs, rr,
):
    owner = lax.axis_index("owner")
    sub = lax.axis_index("sub")
    core = lax.rem(owner, 2)
    sx, sy = sub // SIDE, lax.rem(sub, SIDE)
    a = sx * (1 - core) + sy * core
    c = sy * (1 - core) + sx * core

    def at(ra, rc):
        return (4 * ra + rc) * (1 - core) + (4 * rc + ra) * core

    def ring(v, step):
        return lax.rem(v + step + SIDE, SIDE)

    def rcopy(src, dst, ssem, rsem, dev):
        return pltpu.make_async_remote_copy(
            src_ref=src, dst_ref=dst, send_sem=ssem, recv_sem=rsem,
            device_id=dev, device_id_type=pl.DeviceIdType.MESH,
        )

    barrier = pltpu.get_barrier_semaphore()

    @pl.loop(1, OWN)
    def _(j):
        pl.semaphore_signal(barrier, inc=1, device_id=(lax.rem(owner + j, OWN), sub),
                            device_id_type=pl.DeviceIdType.MESH)

    @pl.loop(1, SUB)
    def _(j):
        pl.semaphore_signal(barrier, inc=1, device_id=(owner, lax.rem(sub + j, SUB)),
                            device_id_type=pl.DeviceIdType.MESH)

    fetches = [
        pltpu.make_async_copy(res_hbm, res_ref, loads.at[0]),
        pltpu.make_async_copy(asm_hbm, asm_ref, loads.at[1]),
        pltpu.make_async_copy(inv_hbm, inv_ref, loads.at[2]),
        pltpu.make_async_copy(mat_hbm, rows_in.at[c], loads.at[3]),
    ]
    for fetch in fetches:
        fetch.start()

    lane = iota((8, LANES), 1)
    low = low_half((8, LANES))

    fetches[0].wait()

    def tile(t):
        return res_ref[:, LANES * t:LANES * (t + 1)]

    for k in range(4):
        tails = None
        for j in range(8):
            g = 8 * k + j
            if j == 0:
                main = tile(g + k)
            else:
                main = pltpu.roll(
                    jnp.where(lane >= 16 * j, tile(g + k), tile(g + k + 1)), LANES - 16 * j, 1
                )
            zmain[g] = main
            nxt = tile(g + k + 1)
            tails = nxt if j == 0 else jnp.where(lane // 16 == j, nxt, tails)
        moved = block_transpose(tails)
        for j in range(8):
            ztail[8 * k + j] = moved[j:j + 1, :]

    fetches[2].wait()
    inv_out[0:BLK] = inv_ref[:, 0:LANES]
    inv_out[BLK:] = jnp.zeros((TAIL, LANES), F32)
    for g in range(BLK // TAIL):
        inv_out[BLK:, 16 * g:16 * (g + 1)] = inv_ref[TAIL * g:TAIL * (g + 1), LANES:BLK]

    fetches[1].wait()
    col = iota((8, SUB * BLK), 1)
    holder_of = col // BLK
    which = jnp.where(iota((8, SUB * BLK), 0) == 0, col - holder_of * BLK, holder_of)
    which = which.astype(F32).astype(BF16)
    info[...] = jnp.zeros_like(info)
    for j in range(4):
        block = asm_ref[:, j, :].astype(F32).astype(BF16)
        info[:, PRIM * j:PRIM * (j + 1)] = dot_nt(which, block)
    place8 = info[...]
    inside = place8.astype(BF16)
    held = place8[1:2, :].astype(jnp.int32)
    dof = iota((1, 256), 1)
    which_sub = ((dof >= PRIM).astype(jnp.int32) + (dof >= 2 * PRIM).astype(jnp.int32)
                 + (dof >= 3 * PRIM).astype(jnp.int32))
    count = jnp.where(which_sub == 0, cnt_ref[0, 0], jnp.where(
        which_sub == 1, cnt_ref[0, 1], jnp.where(which_sub == 2, cnt_ref[0, 2], cnt_ref[0, 3])))
    live = ((dof - PRIM * which_sub) < count) & (dof < BLK)
    held = jnp.where(live, held, -1)
    hot = (held == iota((SUB, 256), 0)).astype(F32)
    upper = (iota((256, 256), 0) < iota((256, 256), 1)).astype(F32).astype(BF16)
    rank = jnp.sum(hot * dot(hot.astype(BF16), upper), axis=0, keepdims=True).astype(jnp.int32)
    hx, hy = held // SIDE, held & 3
    ha = hx * (1 - core) + hy * core
    hk = hy * (1 - core) + hx * core
    spot = ha * LANES + (hk // 2) * HALF + (hk & 1) * SLOT + rank
    spot = jnp.where(live, spot, -1)
    pick[...] = (iota((4 * LANES, 256), 0) == spot).astype(F32).astype(BF16)
    rows = dot_nt(inside, pick[...])
    for j in range(4):
        offs[j] = rows[0:1, LANES * j:LANES * (j + 1)]

    fetches[3].wait()

    pl.semaphore_wait(barrier, OWN - 1 + SUB - 1)

    @pl.loop(1, OWN)
    def _(j):
        peer = lax.rem(owner + j, OWN)
        rcopy(zmain.at[peer], zmain_in.at[owner], zs_m.at[peer], zr_m.at[owner], (peer, sub)).start()
        rcopy(ztail.at[peer], ztail_in.at[owner], zs_t.at[peer], zr_t.at[owner], (peer, sub)).start()

    def off_copy(peer, pa):
        return rcopy(offs.at[pa], offs_in.at[sub], os.at[peer], orr.at[sub], (owner, peer))

    def group_of(peer):
        px, py = peer // SIDE, lax.rem(peer, SIDE)
        return px * (1 - core) + py * core, py * (1 - core) + px * core

    @pl.loop(1, SUB)
    def _(j):
        peer = lax.rem(sub + j, SUB)
        pa, _pc = group_of(peer)
        off_copy(peer, pa).start()

    nextc, prevc = ring(c, 1), ring(c, -1)
    oppc = ring(c, 2)
    c_right, c_left, c_opp = (owner, at(a, nextc)), (owner, at(a, prevc)), (owner, at(a, oppc))
    top, bottom = pl.ds(0, BLK // 2), pl.ds(BLK // 2, BLK // 2)

    def mat_copy(n, slot, part, dev):
        piece = rows_in.at[slot, part]
        return rcopy(piece, piece, ms.at[n], mr.at[n], dev)

    def inv_copy(n, slot, dev):
        return rcopy(inv_out, inv_in.at[slot], ivs.at[n], ivr.at[n], dev)

    mat_copy(0, c, top, c_right).start()
    mat_copy(2, c, bottom, c_left).start()
    mat_copy(1, c, bottom, c_right).start()
    mat_copy(3, c, top, c_left).start()
    for n, dev in ((0, c_right), (1, c_left), (2, c_opp)):
        inv_copy(n, c, dev).start()

    zmain_in[owner] = zmain[owner]
    ztail_in[owner] = ztail[owner]
    offs_in[sub] = offs[a]
    inv_in[c] = inv_out[...]
    vin[:, MSG:HALF, :] = jnp.zeros((SUB, HALF - MSG, LANES), F32)
    back[...] = jnp.zeros_like(back)

    def store_rows(k):
        at_hi = pl.multiple_of(k * BLK, 16)
        at_lo = pl.multiple_of((SIDE + k) * BLK, 16)
        lanes = iota((BLK, LANES), 1)

        @pl.loop(0, SIDE)
        def _(d):
            ra = ring(a, d)

            def window(t, kk):
                start = LANES * t + BLK * (at(ra, kk) - kk)
                first, shift = start // LANES, lax.rem(start, LANES)
                after = jnp.minimum(first + 1, SUB * BLK // LANES - 1)
                one = rows_in[k, :, pl.ds(pl.multiple_of(first * LANES, LANES), LANES)]
                two = rows_in[k, :, pl.ds(pl.multiple_of(after * LANES, LANES), LANES)]
                both = jnp.where(lanes >= shift, one, two)
                return pltpu.roll(both, lax.rem(LANES - shift, LANES), 1)

            for t in range(5):
                ends = [kk for kk in range(SIDE)
                        if BLK * kk < LANES * (t + 1) and BLK * (kk + 1) > LANES * t]
                value = window(t, ends[0])
                if len(ends) > 1:
                    edge = BLK * ends[1] - LANES * t
                    value = jnp.where(lanes < edge, value, window(t, ends[1]))
                hi, lo = split(value)
                cols = slice(LANES * t, LANES * (t + 1))
                stack[d, pl.ds(at_hi, BLK), cols] = hi
                stack[d, pl.ds(at_lo, BLK), cols] = lo

    store_rows(c)

    @pl.loop(1, OWN)
    def _(j):
        peer = lax.rem(owner + j, OWN)
        rcopy(zmain.at[peer], zmain_in.at[peer], zs_m.at[peer], zr_m.at[peer], (peer, sub)).wait_recv()
        rcopy(ztail.at[peer], ztail_in.at[peer], zs_t.at[peer], zr_t.at[peer], (peer, sub)).wait_recv()

    local[:, 0:LANES] = zmain_in[...].reshape(8 * OWN, LANES)
    for k in range(4):
        moved = block_transpose(ztail_in[8 * k:8 * (k + 1)].reshape(8, LANES))
        for j in range(8):
            src = 8 * k + j
            local[8 * src:8 * (src + 1), LANES:] = moved if j == 0 else pltpu.roll(
                moved, LANES - 16 * j, 1)
    loc_hi, loc_lo = split(local[...])
    vals = dot_nt(pick[...], loc_hi) + dot_nt(pick[...], loc_lo)
    low_msg = low_half((MSG, LANES))
    for ra in range(4):
        for t in range(2):
            first = vals[LANES * ra:LANES * ra + MSG, LANES * t:LANES * (t + 1)]
            second = vals[LANES * ra + HALF:LANES * ra + HALF + MSG, LANES * t:LANES * (t + 1)]
            vsend[4 * ra + 2 * t] = jnp.where(low_msg, first, half_swap(second))
            vsend[4 * ra + 2 * t + 1] = jnp.where(low_msg, half_swap(first), second)
    body = pl.ds(0, MSG)

    @pl.loop(1, SUB)
    def _(j):
        peer = lax.rem(sub + j, SUB)
        pa, pc = group_of(peer)
        rcopy(vsend.at[4 * pa + pc], vin.at[sub, body], vs.at[peer], vr.at[sub], (owner, peer)).start()

    vin[sub, body] = vsend[4 * a + c]

    @pl.loop(1, SUB)
    def _(j):
        peer = lax.rem(sub + j, SUB)
        rcopy(offs.at[0], offs_in.at[peer], os.at[peer], orr.at[peer], (owner, peer)).wait_recv()

    lane1 = iota((1, LANES), 1)
    extra = jnp.where((lane1 & (HALF - 1)) >= SLOT, float(BLK), 0.0)
    for m in range(SUB // 2):
        one, two = offs_in[2 * m], offs_in[2 * m + 1]
        for h in range(2):
            if h == 0:
                row = jnp.where(lane1 < HALF, one, half_swap(two)) + extra
            else:
                row = jnp.where(lane1 < HALF, half_swap(one), two) + extra
            rowi = row.astype(jnp.int32)
            cols = pl.ds(LANES * m, LANES)
            land[h, :, cols] = (iota((PACK, LANES), 0) == rowi).astype(F32).astype(BF16)
            down = jnp.broadcast_to(row, (LANES, LANES)).T.astype(jnp.int32)
            for t, width in ((0, LANES), (1, LANES), (2, PACK - 2 * LANES)):
                hit = (down == iota((LANES, LANES), 1) + LANES * t).astype(F32).astype(BF16)
                land_t[h, cols, LANES * t:LANES * t + width] = hit[:, :width]

    mat_copy(0, prevc, top, c_left).wait_recv()
    mat_copy(4, prevc, top, c_right).start()
    mat_copy(2, nextc, bottom, c_right).wait_recv()
    mat_copy(5, nextc, bottom, c_left).start()


    for n, slot in ((0, prevc), (1, nextc), (2, oppc)):
        inv_copy(n, slot, c_right).wait_recv()
    for k in range(4):
        inv_full[k, :, 0:LANES] = inv_in[k, 0:BLK]
        for g in range(BLK // TAIL):
            inv_full[k, TAIL * g:TAIL * (g + 1), LANES:BLK] = inv_in[
                k, BLK:, 16 * g:16 * (g + 1)]
        hi, lo = split(inv_full[k])
        mstack[k, 0:BLK] = hi
        mstack[k, BLK:] = lo

    @pl.loop(1, SUB)
    def _(j):
        peer = lax.rem(sub + j, SUB)
        rcopy(vsend.at[0], vin.at[peer, body], vs.at[peer], vr.at[peer], (owner, peer)).wait_recv()

    low_pack = low_half((PACK, LANES))
    low_blk = low_half((BLK, LANES))

    def side_by_side(x):
        hi, lo = split(x)
        return jnp.concatenate([hi, lo], axis=1)

    def fold(x):
        return x[:, :LANES] + x[:, LANES:]

    values = side_by_side(vin[...].reshape(SUB * HALF, LANES))
    r = jnp.where(low_pack, fold(dot(land[0], values)), fold(dot(land[1], values)))

    def spread(x):
        keep = low_half(x.shape)
        hi = x.astype(BF16).astype(F32)
        rem = x - hi
        mid = rem.astype(BF16).astype(F32)
        lo = rem - mid
        hi_, mid_, lo_ = half_swap(hi), half_swap(mid), half_swap(lo)
        first = (jnp.where(keep, hi, mid_), jnp.where(keep, lo, lo_))
        second = (jnp.where(keep, hi_, mid), jnp.where(keep, lo_, lo))
        return tuple(jnp.concatenate(p, axis=1).astype(BF16) for p in (first, second))

    def gathered(x):
        return x[:, :LANES] + half_swap(x[:, :LANES]) + x[:, LANES:]

    def precond(v):
        parts = spread(v)
        done = []
        for k in range(4):
            lo_row = (k % 2) * BLK
            got = dot(mstack[k], parts[k // 2][lo_row:lo_row + BLK])
            done.append(gathered(got[:BLK] + got[BLK:]))
        return jnp.concatenate(
            [jnp.where(low_blk, done[kk], done[2 + kk]) for kk in range(2)], axis=0)

    nexta, preva, oppa = ring(a, 1), ring(a, -1), ring(a, 2)
    a_right, a_left, a_opp = (owner, at(nexta, c)), (owner, at(preva, c)), (owner, at(oppa, c))
    head, rest = pl.ds(0, CUT), pl.ds(CUT, VEC - CUT)

    def vec_copy(it, n, slot, part, dev, forward=False):
        source = gin.at[it, slot, part] if forward else gsend.at[it, part]
        return rcopy(source, gin.at[it, slot, part], gs.at[it, n], gr.at[it, n], dev)

    def widen(d, x):
        first, second = spread(x)
        wide[d, 0:PACK] = first
        wide[d, PACK:] = second

    def product(d):
        out = []
        for h in range(2):
            got = dot(stack[d, PACK * h:PACK * (h + 1), 0:2 * PACK], wide[d])
            got = got + dot(stack[d, PACK * (2 + h):PACK * (3 + h), 0:2 * PACK], wide[d])
            out.append(gathered(got))
        return jnp.where(low_pack, out[0], out[1])

    def gather_start(it, v, sums):
        gsend[it, 0:PACK] = v
        gsend[it, PACK:VEC] = sums
        vec_copy(it, 0, a, head, a_right).start()
        vec_copy(it, 2, a, rest, a_left).start()
        vec_copy(it, 1, a, rest, a_right).start()
        vec_copy(it, 3, a, head, a_left).start()
        widen(0, v)

    def gather_pass(it):
        vec_copy(it, 0, preva, head, a_left).wait_recv()
        vec_copy(it, 4, preva, head, a_right, True).start()
        vec_copy(it, 2, nexta, rest, a_right).wait_recv()
        vec_copy(it, 5, nexta, rest, a_left, True).start()

    def gather_near(it):
        vec_copy(it, 1, preva, rest, a_left).wait_recv()
        widen(3, gin[it, preva, 0:PACK])
        vec_copy(it, 3, nexta, head, a_right).wait_recv()
        widen(1, gin[it, nexta, 0:PACK])

    def gather_end(it, sums):
        vec_copy(it, 4, oppa, head, a_right).wait_recv()
        vec_copy(it, 5, oppa, rest, a_left).wait_recv()
        widen(2, gin[it, oppa, 0:PACK])
        total = sums
        for ra in (preva, nexta, oppa):
            total = total + gin[it, ra, PACK:VEC]
        return total

    def column_sum(x, y):
        s = jnp.sum(x * y, axis=0, keepdims=True)
        return s + half_swap(s)

    row8 = iota((8, LANES), 0)

    def partial_sums(r, u, w):
        one, two = column_sum(r, u), column_sum(w, u)
        return jnp.where(row8 == 0, one, jnp.where(row8 == 1, two, 0.0))

    u = precond(r)
    nothing = jnp.zeros((8, LANES), F32)
    gather_start(0, u, nothing)
    gather_pass(0)
    gather_near(0)

    mat_copy(1, prevc, bottom, c_left).wait_recv()
    store_rows(prevc)
    mat_copy(3, nextc, top, c_right).wait_recv()
    store_rows(nextc)
    mat_copy(4, oppc, top, c_right).wait_recv()
    mat_copy(5, oppc, bottom, c_left).wait_recv()
    store_rows(oppc)

    gather_end(0, nothing)
    w = product(0) + product(1) + product(2) + product(3)

    gamma = alpha = None
    x = p = s = q = z = None
    for it in range(1, ITERS):
        sums = partial_sums(r, u, w)
        m = precond(w)
        gather_start(it, m, sums)
        partial[...] = product(0)
        gather_pass(it)
        gather_near(it)
        partial[...] = partial[...] + product(1) + product(3)
        total = gather_end(it, sums)
        n = partial[...] + product(2)
        gamma_new, delta = total[0:1], total[1:2]
        if it == 1:
            alpha = gamma_new / delta
            z, q, s, p = n, m, w, u
            x = alpha * p
        else:
            beta = gamma_new / gamma
            alpha = gamma_new / (delta - beta * gamma_new / alpha)
            z, q, s, p = n + beta * z, m + beta * q, w + beta * s, u + beta * p
            x = x + alpha * p
        gamma = gamma_new
        r = r - alpha * s
        u = u - alpha * q
        w = w - alpha * z

    sums = partial_sums(r, u, w)
    ssend[...] = sums
    for n_, dev in ((0, a_right), (1, a_left), (2, a_opp)):
        rcopy(ssend, sin.at[n_], ss.at[n_], sr.at[n_], dev).start()
    total = sums
    for n_ in range(3):
        rcopy(ssend, sin.at[n_], ss.at[n_], sr.at[n_], a_right).wait_recv()
        total = total + sin[n_]
    gamma_new, delta = total[0:1], total[1:2]
    beta = gamma_new / gamma
    alpha = gamma_new / (delta - beta * gamma_new / alpha)
    s, p = w + beta * s, u + beta * p
    x = x + alpha * p
    r = r - alpha * s

    xs = side_by_side(x)
    low_slots = low_half((SUB * HALF, LANES))
    reply = jnp.where(low_slots, fold(dot(land_t[0], xs)), fold(dot(land_t[1], xs)))
    psend[...] = reply.reshape(SUB, HALF, LANES)
    mine = 4 * a + c

    @pl.loop(1, SUB)
    def _(j):
        peer = lax.rem(sub + j, SUB)
        rcopy(psend.at[peer, body], pin.at[mine], ps.at[peer], pr.at[mine], (owner, peer)).start()

    pin[mine] = psend[sub, body]

    rbuf[...] = r
    for n_, slot, dev in ((0, nextc, c_right), (1, prevc, c_left), (2, oppc, c_opp)):
        source = rbuf.at[pl.ds(pl.multiple_of(lax.rem(slot, 2) * BLK, 8), BLK)]
        rcopy(source, rin.at[c], rs.at[n_], rr.at[n_], dev).start()
    rin[c] = rbuf[pl.ds(pl.multiple_of(lax.rem(c, 2) * BLK, 8), BLK)]

    @pl.loop(1, SUB)
    def _(j):
        peer = lax.rem(sub + j, SUB)
        pa, pc = group_of(peer)
        slot = 4 * pa + pc
        rcopy(psend.at[peer, body], pin.at[slot], ps.at[peer], pr.at[slot], (owner, peer)).wait_recv()

    for ra in range(4):
        for t in range(2):
            one, two = pin[4 * ra + 2 * t], pin[4 * ra + 2 * t + 1]
            cols = slice(LANES * t, LANES * (t + 1))
            back[LANES * ra:LANES * ra + MSG, cols] = jnp.where(low_msg, one, half_swap(two))
            back[LANES * ra + HALF:LANES * ra + HALF + MSG, cols] = jnp.where(
                low_msg, half_swap(one), two)
    back_hi, back_lo = split(back[...])
    mine_back = dot_tn(back_hi, pick[...]) + dot_tn(back_lo, pick[...])
    cmain[...] = mine_back[:, :LANES].reshape(OWN, 8, LANES)
    for k in range(4):
        tails = None
        for j in range(8):
            src = 8 * k + j
            piece = mine_back[8 * src:8 * (src + 1), LANES:]
            tails = piece if j == 0 else tails + pltpu.roll(piece, 16 * j, 1)
        moved = block_transpose(tails)
        for j in range(8):
            ctail[8 * k + j] = moved[j:j + 1, :]

    @pl.loop(1, OWN)
    def _(j):
        peer = lax.rem(owner + j, OWN)
        rcopy(cmain.at[peer], cmain_in.at[owner], cs_m.at[peer], cr_m.at[owner], (peer, sub)).start()
        rcopy(ctail.at[peer], ctail_in.at[owner], cs_t.at[peer], cr_t.at[owner], (peer, sub)).start()

    cmain_in[owner] = cmain[owner]
    ctail_in[owner] = ctail[owner]

    for n_, slot in ((0, prevc), (1, nextc), (2, oppc)):
        rcopy(rbuf.at[pl.ds(0, BLK)], rin.at[slot], rs.at[n_], rr.at[n_], c_right).wait_recv()
    for t in range(2):
        one, two = rin[2 * t], rin[2 * t + 1]
        upper_half = jnp.where(low_blk, half_swap(one), two)
        lower_half = jnp.where(low_blk, one, half_swap(two))
        resid_ref[:, LANES * t:LANES * (t + 1)] = jnp.where(c < 2, lower_half, upper_half)

    for n_ in range(6):
        mat_copy(n_, c, top, c_right).wait_send()
        for it in range(ITERS):
            part = head if n_ in (0, 3, 4) else rest
            vec_copy(it, n_, a, part, a_right).wait_send()
    for n_ in range(3):
        inv_copy(n_, c, c_right).wait_send()
        rcopy(ssend, sin.at[n_], ss.at[n_], sr.at[n_], a_right).wait_send()
        rcopy(rbuf.at[pl.ds(0, BLK)], rin.at[c], rs.at[n_], rr.at[n_], c_right).wait_send()

    @pl.loop(1, SUB)
    def _(j):
        peer = lax.rem(sub + j, SUB)
        rcopy(offs.at[0], offs_in.at[peer], os.at[peer], orr.at[peer], (owner, peer)).wait_send()
        rcopy(vsend.at[0], vin.at[peer, body], vs.at[peer], vr.at[peer], (owner, peer)).wait_send()
        rcopy(psend.at[peer, body], pin.at[peer], ps.at[peer], pr.at[peer], (owner, peer)).wait_send()

    @pl.loop(1, OWN)
    def _(j):
        peer = lax.rem(owner + j, OWN)
        rcopy(zmain.at[peer], zmain_in.at[peer], zs_m.at[peer], zr_m.at[peer], (peer, sub)).wait_send()
        rcopy(ztail.at[peer], ztail_in.at[peer], zs_t.at[peer], zr_t.at[peer], (peer, sub)).wait_send()
        rcopy(cmain.at[peer], cmain_in.at[peer], cs_m.at[peer], cr_m.at[peer], (peer, sub)).wait_recv()
        rcopy(ctail.at[peer], ctail_in.at[peer], cs_t.at[peer], cr_t.at[peer], (peer, sub)).wait_recv()

    @pl.loop(1, OWN)
    def _(j):
        peer = lax.rem(owner + j, OWN)
        rcopy(cmain.at[peer], cmain_in.at[peer], cs_m.at[peer], cr_m.at[peer], (peer, sub)).wait_send()
        rcopy(ctail.at[peer], ctail_in.at[peer], cs_t.at[peer], cr_t.at[peer], (peer, sub)).wait_send()

    for k in range(4):
        tails = block_transpose(ctail_in[8 * k:8 * (k + 1)].reshape(8, LANES))
        turned = [
            cmain_in[8 * k + j] if j == 0 else pltpu.roll(cmain_in[8 * k + j], 16 * j, 1)
            for j in range(8)
        ]
        for m in range(9):
            if m == 0:
                value = turned[0]
            else:
                value = jnp.where(lane < 16 * m, tails, turned[m]) if m < 8 else tails
                value = jnp.where(lane < 16 * (m - 1), turned[m - 1], value)
            where_to = LANES * (9 * k + m)
            corr_ref[:, where_to:where_to + LANES] = value


def hand_on(corr_in, resid_in, corr_out, resid_out):
    corr_out[...] = corr_in[...]
    resid_out[...] = resid_in[...]


def shards(residual, counts, assembly, level_two, block_inverse):
    vmem = pl.BlockSpec(memory_space=pltpu.VMEM)
    smem = pl.BlockSpec(memory_space=pltpu.SMEM)
    anywhere = pl.BlockSpec(memory_space=pl.ANY)
    V = pltpu.VMEM
    dma = pltpu.SemaphoreType.DMA
    scratch = [
        V(residual.shape, F32), V((PRIM, SIDE, SUB * BLK), jnp.int32), V((BLK, BLK), F32),
        V((BLK + TAIL, LANES), F32),
        V((OWN, 8, LANES), F32), V((OWN, 1, LANES), F32),
        V((OWN, 8, LANES), F32), V((OWN, 1, LANES), F32),
        V((OWN, 8, LANES), F32), V((OWN, 1, LANES), F32),
        V((OWN, 8, LANES), F32), V((OWN, 1, LANES), F32),
        V((SIDE, 1, LANES), F32), V((SUB, 1, LANES), F32), V((8, 256), F32),
        V((SIDE, BLK, SUB * BLK), F32), V((SIDE, BLK + TAIL, LANES), F32),
        V((SIDE, BLK, BLK), F32),
        V((SIDE, 2 * SIDE * BLK, 5 * LANES), BF16), V((SIDE, 2 * BLK, BLK), BF16),
        V((SUB, MSG, LANES), F32), V((SUB, HALF, LANES), F32),
        V((2, PACK, SUB * HALF), BF16), V((2, SUB * HALF, PACK), BF16), V((4 * LANES, 256), BF16),
        V((ITERS, VEC, LANES), F32), V((ITERS, SIDE, VEC, LANES), F32),
        V((SIDE, SIDE * BLK, 2 * LANES), BF16), V((8, LANES), F32), V((3, 8, LANES), F32),
        V((SUB, HALF, LANES), F32), V((SUB, MSG, LANES), F32), V((4 * LANES, 256), F32),
        V((PACK, LANES), F32), V((SIDE, BLK, LANES), F32), V((256, 256), F32), V((PACK, LANES), F32),
        dma((4,)),
        dma((OWN,)), dma((OWN,)), dma((OWN,)), dma((OWN,)),
        dma((OWN,)), dma((OWN,)), dma((OWN,)), dma((OWN,)),
        dma((SUB,)), dma((SUB,)), dma((6,)), dma((6,)), dma((3,)), dma((3,)),
        dma((SUB,)), dma((SUB,)), dma((ITERS, 6)), dma((ITERS, 6)), dma((3,)), dma((3,)),
        dma((SUB,)), dma((SUB,)), dma((3,)), dma((3,)),
    ]
    corr, resid = pl.pallas_call(
        kernel,
        out_shape=(
            jax.ShapeDtypeStruct(residual.shape, F32),
            jax.ShapeDtypeStruct((BLK, 8 * OWN), F32),
        ),
        in_specs=[smem, anywhere, anywhere, anywhere, anywhere],
        out_specs=(vmem, vmem),
        scratch_shapes=scratch,
        compiler_params=pltpu.CompilerParams(
            collective_id=0, has_side_effects=True, vmem_limit_bytes=44 * 1024 * 1024
        ),
    )(counts, residual, jnp.transpose(assembly[0], (1, 0, 2)), level_two[0], block_inverse[0])
    corr, resid = pl.pallas_call(
        hand_on,
        out_shape=(
            jax.ShapeDtypeStruct(corr.shape, F32), jax.ShapeDtypeStruct(resid.shape, F32)
        ),
        in_specs=[vmem, vmem],
        out_specs=(vmem, vmem),
    )(corr, resid)
    return corr, resid[None]


def solution(mesh):
    in_specs = (
        P("owner", "sub"),
        P("owner", "sub"),
        P("owner", "sub", None, None),
        P("owner", "sub", None),
        P("owner", "sub", None),
    )
    out_specs = (P("owner", "sub"), P("owner", "sub", None))
    return jax.shard_map(shards, mesh=mesh, in_specs=in_specs, out_specs=out_specs, check_vma=False)
```

```python
import jax
import jax.numpy as jnp
from jax import lax
from jax.experimental import pallas as pl
from jax.experimental.pallas import tpu as pltpu
from jax.sharding import PartitionSpec as P

ITERS = 4
F32 = jnp.float32
BF16 = jnp.bfloat16
OWN = 32
SUB = 16
SIDE = 4
BLK = 144
SLOT = 18
PRIM = 36
LANES = 128
HALF = 64
PACK = 2 * BLK
MSG = 40
VEC = PACK + 8
TAIL = 24
CUTS = (0, 72, 224, VEC)


def iota(shape, dim):
    return lax.broadcasted_iota(jnp.int32, shape, dim)


def dot(a, b):
    return jnp.dot(a, b, preferred_element_type=F32)


def dot_nt(a, b):
    return lax.dot_general(a, b, (((1,), (1,)), ((), ())), preferred_element_type=F32)


def split(x):
    hi = x.astype(BF16)
    return hi, (x - hi.astype(F32)).astype(BF16)


def half_swap(x):
    return pltpu.roll(x, HALF, 1)


def low_half(shape):
    return iota(shape, 1) < HALF


def block_transpose(t):
    away = iota((8, LANES), 0) - iota((8, LANES), 1) // 16
    out = t
    for shift in range(1, 8):
        moved = pltpu.roll(pltpu.roll(t, shift, 0), LANES - 16 * shift, 1)
        out = jnp.where((away & 7) == shift, moved, out)
    return out


def kernel(
    cnt_hbm, res_hbm, asm_hbm, mat_hbm, inv_hbm,
    corr_ref, resid_ref,
    cnt_ref, res_ref, asm_ref, inv_ref, inv_out,
    zmain, ztail, zmain_in, ztail_in,
    cmain, ctail, cmain_in, ctail_in,
    offs, offs_in, info,
    rows_in, inv_in, inv_full, stack, mstack,
    vsend, vin, land, land_t, pick, pick_t,
    gsend, gin, wide, ssend, sin,
    psend, pin, back, rbuf, rin, local, partial, by_rows, answers,
    loads,
    zs_m, zr_m, zs_t, zr_t, cs_m, cr_m, cs_t, cr_t,
    os, orr, ms, mr, ivs, ivr, vs, vr, gs, gr, ss, sr, ps, pr, rs, rr,
):
    owner = lax.axis_index("owner")
    sub = lax.axis_index("sub")
    core = lax.rem(owner, 2)
    sx, sy = sub // SIDE, lax.rem(sub, SIDE)
    a = sx * (1 - core) + sy * core
    c = sy * (1 - core) + sx * core

    def at(ra, rc):
        return (4 * ra + rc) * (1 - core) + (4 * rc + ra) * core

    def ring(v, step):
        return lax.rem(v + step + SIDE, SIDE)

    def rcopy(src, dst, ssem, rsem, dev):
        return pltpu.make_async_remote_copy(
            src_ref=src, dst_ref=dst, send_sem=ssem, recv_sem=rsem,
            device_id=dev, device_id_type=pl.DeviceIdType.MESH,
        )

    barrier = pltpu.get_barrier_semaphore()

    def each_owner(act):
        act((owner + OWN // 2) & (OWN - 1))

        @pl.loop(1, OWN // 2)
        def _(i):
            act((owner + (OWN // 2 + i)) & (OWN - 1))
            act((owner + (OWN // 2 - i)) & (OWN - 1))

    def greet(dev):
        pl.semaphore_signal(barrier, inc=1, device_id=dev, device_id_type=pl.DeviceIdType.MESH)

    each_owner(lambda peer: greet((peer, sub)))

    @pl.loop(1, SUB)
    def _(j):
        greet((owner, (sub + j) & (SUB - 1)))

    fetches = [
        pltpu.make_async_copy(res_hbm, res_ref, loads.at[0]),
        pltpu.make_async_copy(asm_hbm, asm_ref, loads.at[1]),
        pltpu.make_async_copy(inv_hbm, inv_ref, loads.at[2]),
        pltpu.make_async_copy(mat_hbm, rows_in.at[c], loads.at[3]),
        pltpu.make_async_copy(cnt_hbm, cnt_ref, loads.at[4]),
    ]
    for fetch in fetches:
        fetch.start()

    lane = iota((8, LANES), 1)
    low = low_half((8, LANES))

    fetches[0].wait()

    def tile(t):
        return res_ref[:, LANES * t:LANES * (t + 1)]

    for k in range(4):
        tails = None
        for j in range(8):
            g = 8 * k + j
            if j == 0:
                main = tile(g + k)
            else:
                main = pltpu.roll(
                    jnp.where(lane >= 16 * j, tile(g + k), tile(g + k + 1)), LANES - 16 * j, 1
                )
            zmain[g] = main
            nxt = tile(g + k + 1)
            tails = nxt if j == 0 else jnp.where(lane // 16 == j, nxt, tails)
        moved = block_transpose(tails)
        for j in range(8):
            ztail[8 * k + j] = moved[j:j + 1, :]

    fetches[2].wait()
    inv_out[0:BLK] = inv_ref[:, 0:LANES]
    inv_out[BLK:] = jnp.zeros((TAIL, LANES), F32)
    for g in range(BLK // TAIL):
        inv_out[BLK:, 16 * g:16 * (g + 1)] = inv_ref[TAIL * g:TAIL * (g + 1), LANES:BLK]

    fetches[1].wait()
    fetches[4].wait()
    col = iota((8, SUB * BLK), 1)
    holder_of = col // BLK
    which = jnp.where(iota((8, SUB * BLK), 0) == 0, col - holder_of * BLK, holder_of)
    which = which.astype(F32).astype(BF16)
    info[...] = jnp.zeros_like(info)
    for j in range(4):
        block = asm_ref[:, j, :].astype(F32).astype(BF16)
        info[:, PRIM * j:PRIM * (j + 1)] = dot_nt(which, block)
    place8 = info[...]
    inside = place8.astype(BF16)
    held = place8[1:2, :].astype(jnp.int32)
    dof = iota((1, 256), 1)
    which_sub = ((dof >= PRIM).astype(jnp.int32) + (dof >= 2 * PRIM).astype(jnp.int32)
                 + (dof >= 3 * PRIM).astype(jnp.int32))
    count = jnp.where(which_sub == 0, cnt_ref[0, 0], jnp.where(
        which_sub == 1, cnt_ref[0, 1], jnp.where(which_sub == 2, cnt_ref[0, 2], cnt_ref[0, 3])))
    live = ((dof - PRIM * which_sub) < count) & (dof < BLK)
    held = jnp.where(live, held, -1)
    hot = (held == iota((SUB, 256), 0)).astype(F32)
    upper = (iota((256, 256), 0) < iota((256, 256), 1)).astype(F32).astype(BF16)
    rank = jnp.sum(hot * dot(hot.astype(BF16), upper), axis=0, keepdims=True).astype(jnp.int32)
    hx, hy = held // SIDE, held & 3
    ha = hx * (1 - core) + hy * core
    hk = hy * (1 - core) + hx * core
    spot = ha * LANES + (hk // 2) * HALF + (hk & 1) * SLOT + rank
    spot = jnp.where(live, spot, -1)
    pick[...] = (iota((4 * LANES, 256), 0) == spot).astype(F32).astype(BF16)
    rows = dot_nt(inside, pick[...])
    for j in range(4):
        offs[j] = rows[0:1, LANES * j:LANES * (j + 1)]

    fetches[3].wait()

    pl.semaphore_wait(barrier, OWN - 1 + SUB - 1)

    def group_of(peer):
        px, py = peer // SIDE, lax.rem(peer, SIDE)
        return px * (1 - core) + py * core, py * (1 - core) + px * core

    @pl.loop(1, SUB)
    def _(j):
        peer = lax.rem(sub + j, SUB)
        pa, _pc = group_of(peer)
        rcopy(offs.at[pa], offs_in.at[sub], os, orr, (owner, peer)).start()

    nextc, prevc, oppc = ring(c, 1), ring(c, -1), ring(c, 2)
    c_right, c_left, c_opp = (owner, at(a, nextc)), (owner, at(a, prevc)), (owner, at(a, oppc))
    half = BLK // 2
    top, bottom = pl.ds(0, half), pl.ds(half, half)
    cuts = [top, bottom, bottom, top] + [
        pl.ds(start + at_row, rows) for start in (0, half)
        for at_row, rows in ((0, 40), (40, 32))]

    def mat_copy(n, slot, dev):
        piece = rows_in.at[slot, cuts[n]]
        return rcopy(piece, piece, ms, mr.at[n], dev)

    for dev in (c_opp, c_right, c_left):
        rcopy(inv_out, inv_in.at[c], ivs, ivr, dev).start()
    for n in range(2):
        mat_copy(n, c, c_right).start()
        mat_copy(2 + n, c, c_left).start()

    def send_residual(peer):
        rcopy(zmain.at[peer], zmain_in.at[owner], zs_m, zr_m, (peer, sub)).start()
        rcopy(ztail.at[peer], ztail_in.at[owner], zs_t, zr_t, (peer, sub)).start()

    each_owner(send_residual)

    others, peers, three = pl.ds(0, OWN - 1), pl.ds(0, SUB - 1), pl.ds(0, SIDE - 1)
    z_main = rcopy(zmain.at[others], zmain_in.at[others], zs_m, zr_m, c_right)
    z_tail = rcopy(ztail.at[others], ztail_in.at[others], zs_t, zr_t, c_right)
    all_offs = rcopy(offs_in.at[peers], offs_in.at[peers], os, orr, c_right)
    all_inv = rcopy(inv_in.at[three], inv_in.at[three], ivs, ivr, c_right)

    zmain_in[owner] = zmain[owner]
    ztail_in[owner] = ztail[owner]
    offs_in[sub] = offs[a]
    inv_in[c] = inv_out[...]
    vin[:, MSG:HALF, :] = jnp.zeros((SUB, HALF - MSG, LANES), F32)
    back[...] = jnp.zeros_like(back)

    def store_rows(k):
        at_hi = pl.multiple_of(k * BLK, 16)
        at_lo = pl.multiple_of((SIDE + k) * BLK, 16)
        lanes = iota((BLK, LANES), 1)

        @pl.loop(0, SIDE)
        def _(d):
            ra = ring(a, d)

            def window(t, kk):
                start = LANES * t + BLK * (at(ra, kk) - kk)
                first, shift = start // LANES, lax.rem(start, LANES)
                after = jnp.minimum(first + 1, SUB * BLK // LANES - 1)
                one = rows_in[k, :, pl.ds(pl.multiple_of(first * LANES, LANES), LANES)]
                two = rows_in[k, :, pl.ds(pl.multiple_of(after * LANES, LANES), LANES)]
                both = jnp.where(lanes >= shift, one, two)
                return pltpu.roll(both, lax.rem(LANES - shift, LANES), 1)

            for t in range(5):
                ends = [kk for kk in range(SIDE)
                        if BLK * kk < LANES * (t + 1) and BLK * (kk + 1) > LANES * t]
                value = window(t, ends[0])
                if len(ends) > 1:
                    edge = BLK * ends[1] - LANES * t
                    value = jnp.where(lanes < edge, value, window(t, ends[1]))
                hi, lo = split(value)
                cols = slice(LANES * t, LANES * (t + 1))
                stack[d, pl.ds(at_hi, BLK), cols] = hi
                stack[d, pl.ds(at_lo, BLK), cols] = lo

    store_rows(c)

    z_main.wait_recv()
    z_tail.wait_recv()

    local[:, 0:LANES] = zmain_in[...].reshape(8 * OWN, LANES)
    for k in range(4):
        moved = block_transpose(ztail_in[8 * k:8 * (k + 1)].reshape(8, LANES))
        for j in range(8):
            src = 8 * k + j
            local[8 * src:8 * (src + 1), LANES:] = moved if j == 0 else pltpu.roll(
                moved, LANES - 16 * j, 1)
    loc_hi, loc_lo = split(local[...])
    vals = dot_nt(pick[...], loc_hi) + dot_nt(pick[...], loc_lo)
    low_msg = low_half((MSG, LANES))
    for ra in range(4):
        for t in range(2):
            first = vals[LANES * ra:LANES * ra + MSG, LANES * t:LANES * (t + 1)]
            second = vals[LANES * ra + HALF:LANES * ra + HALF + MSG, LANES * t:LANES * (t + 1)]
            vsend[4 * ra + 2 * t] = jnp.where(low_msg, first, half_swap(second))
            vsend[4 * ra + 2 * t + 1] = jnp.where(low_msg, half_swap(first), second)
    body = pl.ds(0, MSG)

    far = sorted(((da, dc) for da in range(4) for dc in range(4) if da or dc),
                 key=lambda d: -(min(d[0], 4 - d[0]) + min(d[1], 4 - d[1])))
    for da, dc in far:
        pa, pc = ring(a, da), ring(c, dc)
        rcopy(vsend.at[4 * pa + pc], vin.at[sub, body], vs, vr, (owner, at(pa, pc))).start()
    all_vals = rcopy(vin.at[peers, body], vin.at[peers, body], vs, vr, c_right)

    vin[sub, body] = vsend[4 * a + c]

    all_offs.wait_recv()

    pick_t[...] = pick[...].astype(F32).T.astype(BF16)

    lane1 = iota((1, LANES), 1)
    extra = jnp.where((lane1 & (HALF - 1)) >= SLOT, float(BLK), 0.0)
    for m in range(SUB // 2):
        one, two = offs_in[2 * m], offs_in[2 * m + 1]
        for h in range(2):
            if h == 0:
                row = jnp.where(lane1 < HALF, one, half_swap(two)) + extra
            else:
                row = jnp.where(lane1 < HALF, half_swap(one), two) + extra
            rowi = row.astype(jnp.int32)
            cols = pl.ds(LANES * m, LANES)
            land[h, :, cols] = (iota((PACK, LANES), 0) == rowi).astype(F32).astype(BF16)
            down = jnp.broadcast_to(row, (LANES, LANES)).T.astype(jnp.int32)
            for t, width in ((0, LANES), (1, LANES), (2, PACK - 2 * LANES)):
                hit = (down == iota((LANES, LANES), 1) + LANES * t).astype(F32).astype(BF16)
                land_t[h, cols, LANES * t:LANES * t + width] = hit[:, :width]

    mat_copy(0, prevc, c_left).wait_recv()
    mat_copy(4, prevc, c_right).start()
    mat_copy(2, nextc, c_right).wait_recv()
    mat_copy(6, nextc, c_left).start()


    all_inv.wait_recv()
    for k in range(4):
        inv_full[k, :, 0:LANES] = inv_in[k, 0:BLK]
        for g in range(BLK // TAIL):
            inv_full[k, TAIL * g:TAIL * (g + 1), LANES:BLK] = inv_in[
                k, BLK:, 16 * g:16 * (g + 1)]
        hi, lo = split(inv_full[k])
        mstack[k, 0:BLK] = hi
        mstack[k, BLK:] = lo

    mat_copy(1, prevc, c_left).wait_recv()
    store_rows(prevc)
    mat_copy(3, nextc, c_right).wait_recv()
    store_rows(nextc)

    all_vals.wait_recv()

    low_pack = low_half((PACK, LANES))
    low_blk = low_half((BLK, LANES))

    def side_by_side(x):
        hi, lo = split(x)
        return jnp.concatenate([hi, lo], axis=1)

    def fold(x):
        return x[:, :LANES] + x[:, LANES:]

    values = side_by_side(vin[...].reshape(SUB * HALF, LANES))
    r = jnp.where(low_pack, fold(dot(land[0], values)), fold(dot(land[1], values)))

    def spread(x):
        keep = low_half(x.shape)
        hi = x.astype(BF16).astype(F32)
        rem = x - hi
        mid = rem.astype(BF16).astype(F32)
        lo = rem - mid
        mid_ = half_swap(mid)
        first = (jnp.where(keep, hi, mid_), jnp.where(keep, lo, 0.0))
        second = (jnp.where(keep, mid_, hi), jnp.where(keep, 0.0, lo))
        return tuple(jnp.concatenate(p, axis=1).astype(BF16) for p in (first, second))

    def gathered(x):
        one = x[:, :LANES] + x[:, LANES:]
        return one + half_swap(one)

    def precond(v):
        parts = spread(v)
        done = []
        for k in range(4):
            lo_row = (k % 2) * BLK
            got = dot(mstack[k], parts[k // 2][lo_row:lo_row + BLK])
            done.append(gathered(got[:BLK] + got[BLK:]))
        return jnp.concatenate(
            [jnp.where(low_blk, done[kk], done[2 + kk]) for kk in range(2)], axis=0)

    nexta, preva, oppa = ring(a, 1), ring(a, -1), ring(a, 2)
    a_right, a_left, a_opp = (owner, at(nexta, c)), (owner, at(preva, c)), (owner, at(oppa, c))
    head, middle, tail = (pl.ds(CUTS[i], CUTS[i + 1] - CUTS[i]) for i in range(3))
    parts = [head, pl.ds(CUTS[1], VEC - CUTS[1]), tail, pl.ds(0, CUTS[2]), middle, head, tail]
    toward = [a_right, a_right, a_left, a_left, a_opp, a_right, a_left]

    def vec_copy(it, n, slot):
        part = parts[n]
        source = gin.at[it, slot, part] if n > 4 else gsend.at[it, part]
        return rcopy(source, gin.at[it, slot, part], gs.at[it], gr.at[it % 2, n], toward[n])

    def widen(d, x):
        first, second = spread(x)
        wide[d, 0:PACK] = first
        wide[d, PACK:] = second

    def product(d):
        out = []
        for h in range(2):
            got = dot(stack[d, PACK * h:PACK * (h + 1), 0:2 * PACK], wide[d])
            got = got + dot(stack[d, PACK * (2 + h):PACK * (3 + h), 0:2 * PACK], wide[d])
            out.append(gathered(got))
        return jnp.where(low_pack, out[0], out[1])

    def product_rows(k, chunks):
        got = None
        for d in chunks:
            for first in (k, SIDE + k):
                rows = stack[d, pl.ds(pl.multiple_of(first * BLK, 16), BLK), 0:2 * PACK]
                term = dot(rows, wide[d])
                got = term if got is None else got + term
        got = gathered(got)
        by_rows[k] = got if chunks[0] == 0 else by_rows[k] + got

    def gather_start(it, v, sums):
        gsend[it, 0:PACK] = v
        gsend[it, PACK:VEC] = sums
        for n in (0, 2, 1, 3, 4):
            vec_copy(it, n, a).start()
        widen(0, v)

    def gather_pass(it):
        vec_copy(it, 0, preva).wait_recv()
        vec_copy(it, 5, preva).start()
        vec_copy(it, 2, nexta).wait_recv()
        vec_copy(it, 6, nexta).start()

    def gather_near(it):
        vec_copy(it, 1, preva).wait_recv()
        widen(3, gin[it, preva, 0:PACK])
        vec_copy(it, 3, nexta).wait_recv()
        widen(1, gin[it, nexta, 0:PACK])

    def gather_end(it, sums):
        for n in (4, 5, 6):
            vec_copy(it, n, oppa).wait_recv()
        widen(2, gin[it, oppa, 0:PACK])
        total = sums
        for ra in (preva, nexta, oppa):
            total = total + gin[it, ra, PACK:VEC]
        return total

    def column_sum(x, y):
        s = jnp.sum(x * y, axis=0, keepdims=True)
        return s + half_swap(s)

    row8 = iota((8, LANES), 0)

    def partial_sums(r, u, w):
        one, two = column_sum(r, u), column_sum(w, u)
        return jnp.where(row8 == 0, one, jnp.where(row8 == 1, two, 0.0))

    u = precond(r)
    nothing = jnp.zeros((8, LANES), F32)
    gather_start(0, u, nothing)
    mat_copy(5, prevc, c_right).start()
    mat_copy(7, nextc, c_left).start()
    for k in (c, prevc, nextc):
        product_rows(k, (0,))
    gather_pass(0)
    gather_near(0)
    for k in (c, prevc, nextc):
        product_rows(k, (1, 3))
    gather_end(0, nothing)
    for k in (c, prevc, nextc):
        product_rows(k, (2,))
    for n in range(4, 8):
        mat_copy(n, oppc, c_right).wait_recv()
    store_rows(oppc)
    product_rows(oppc, (0, 1, 3, 2))
    w = jnp.concatenate(
        [jnp.where(low_blk, by_rows[kk], by_rows[2 + kk]) for kk in range(2)], axis=0)

    gamma = alpha = None
    x = p = s = q = z = None
    for it in range(1, ITERS):
        sums = partial_sums(r, u, w)
        m = precond(w)
        gather_start(it, m, sums)
        partial[...] = product(0)
        gather_pass(it)
        gather_near(it)
        partial[...] = partial[...] + product(1) + product(3)
        total = gather_end(it, sums)
        n = partial[...] + product(2)
        gamma_new, delta = total[0:1], total[1:2]
        if it == 1:
            alpha = gamma_new / delta
            z, q, s, p = n, m, w, u
            x = alpha * p
        else:
            beta = gamma_new / gamma
            alpha = gamma_new / (delta - beta * gamma_new / alpha)
            z, q, s, p = n + beta * z, m + beta * q, w + beta * s, u + beta * p
            x = x + alpha * p
        gamma = gamma_new
        r = r - alpha * s
        u = u - alpha * q
        w = w - alpha * z

    sums = partial_sums(r, u, w)
    ssend[...] = sums
    for n, dev in ((2, a_opp), (0, a_right), (1, a_left)):
        rcopy(ssend, sin.at[n], ss, sr, dev).start()
    all_sums = rcopy(sin, sin, ss, sr, a_right)

    low_slots = low_half((SUB * HALF, LANES))

    def reply_of(v):
        vs_ = side_by_side(v)
        return jnp.where(low_slots, fold(dot(land_t[0], vs_)), fold(dot(land_t[1], vs_)))

    for n, v in ((0, x), (1, u), (2, p)):
        answers[n] = reply_of(v)
    all_sums.wait_recv()
    total = sums + sin[0] + sin[1] + sin[2]
    gamma_new, delta = total[0:1], total[1:2]
    beta = gamma_new / gamma
    alpha = gamma_new / (delta - beta * gamma_new / alpha)
    reply = answers[0] + alpha * (answers[1] + beta * answers[2])
    psend[...] = reply.reshape(SUB, HALF, LANES)
    mine = 4 * a + c

    for da, dc in far:
        peer = at(ring(a, da), ring(c, dc))
        rcopy(psend.at[peer, body], pin.at[mine], ps, pr, (owner, peer)).start()
    all_back = rcopy(pin.at[peers], pin.at[peers], ps, pr, c_right)

    pin[mine] = psend[sub, body]

    rbuf[...] = r - alpha * (w + beta * s)
    for slot, dev in ((oppc, c_opp), (nextc, c_right), (prevc, c_left)):
        source = rbuf.at[pl.ds(pl.multiple_of(lax.rem(slot, 2) * BLK, 8), BLK)]
        rcopy(source, rin.at[c], rs, rr, dev).start()
    all_resid = rcopy(rin.at[three], rin.at[three], rs, rr, c_right)
    rin[c] = rbuf[pl.ds(pl.multiple_of(lax.rem(c, 2) * BLK, 8), BLK)]

    all_back.wait_recv()

    for ra in range(4):
        for t in range(2):
            one, two = pin[4 * ra + 2 * t], pin[4 * ra + 2 * t + 1]
            cols = slice(LANES * t, LANES * (t + 1))
            back[LANES * ra:LANES * ra + MSG, cols] = jnp.where(low_msg, one, half_swap(two))
            back[LANES * ra + HALF:LANES * ra + HALF + MSG, cols] = jnp.where(
                low_msg, half_swap(one), two)
    back_hi, back_lo = split(back[...])
    mine_back = (dot(pick_t[...], back_hi) + dot(pick_t[...], back_lo)).T
    cmain[...] = mine_back[:, :LANES].reshape(OWN, 8, LANES)
    for k in range(4):
        tails = None
        for j in range(8):
            src = 8 * k + j
            piece = mine_back[8 * src:8 * (src + 1), LANES:]
            tails = piece if j == 0 else tails + pltpu.roll(piece, 16 * j, 1)
        moved = block_transpose(tails)
        for j in range(8):
            ctail[8 * k + j] = moved[j:j + 1, :]

    def send_correction(peer):
        rcopy(cmain.at[peer], cmain_in.at[owner], cs_m, cr_m, (peer, sub)).start()
        rcopy(ctail.at[peer], ctail_in.at[owner], cs_t, cr_t, (peer, sub)).start()

    each_owner(send_correction)

    c_main = rcopy(cmain.at[others], cmain_in.at[others], cs_m, cr_m, c_right)
    c_tail = rcopy(ctail.at[others], ctail_in.at[others], cs_t, cr_t, c_right)

    cmain_in[owner] = cmain[owner]
    ctail_in[owner] = ctail[owner]

    all_resid.wait_recv()
    for t in range(2):
        one, two = rin[2 * t], rin[2 * t + 1]
        upper_half = jnp.where(low_blk, half_swap(one), two)
        lower_half = jnp.where(low_blk, one, half_swap(two))
        resid_ref[:, LANES * t:LANES * (t + 1)] = jnp.where(c < 2, lower_half, upper_half)

    rcopy(rows_in.at[three], rows_in.at[three], ms, mr.at[0], c_right).wait_send()
    for it in range(ITERS):
        rcopy(gin.at[it, three], gin.at[it, three], gs.at[it], gr.at[0, 0], c_right).wait_send()
    for sent in (z_main, z_tail, all_offs, all_inv, all_vals, all_sums, all_back, all_resid):
        sent.wait_send()
    c_main.wait_recv()
    c_tail.wait_recv()
    c_main.wait_send()
    c_tail.wait_send()

    for k in range(4):
        tails = block_transpose(ctail_in[8 * k:8 * (k + 1)].reshape(8, LANES))
        turned = [
            cmain_in[8 * k + j] if j == 0 else pltpu.roll(cmain_in[8 * k + j], 16 * j, 1)
            for j in range(8)
        ]
        for m in range(9):
            if m == 0:
                value = turned[0]
            else:
                value = jnp.where(lane < 16 * m, tails, turned[m]) if m < 8 else tails
                value = jnp.where(lane < 16 * (m - 1), turned[m - 1], value)
            where_to = LANES * (9 * k + m)
            corr_ref[:, where_to:where_to + LANES] = value


def hand_on(corr_in, resid_in, corr_out, resid_out):
    corr_out[...] = corr_in[...]
    resid_out[...] = resid_in[...]


def shards(residual, counts, assembly, level_two, block_inverse):
    vmem = pl.BlockSpec(memory_space=pltpu.VMEM)
    anywhere = pl.BlockSpec(memory_space=pl.ANY)
    V = pltpu.VMEM
    dma = pltpu.SemaphoreType.DMA
    scratch = [
        pltpu.SMEM(counts.shape, jnp.int32),
        V(residual.shape, F32), V((PRIM, SIDE, SUB * BLK), jnp.int32), V((BLK, BLK), F32),
        V((BLK + TAIL, LANES), F32),
        V((OWN, 8, LANES), F32), V((OWN, 1, LANES), F32),
        V((OWN, 8, LANES), F32), V((OWN, 1, LANES), F32),
        V((OWN, 8, LANES), F32), V((OWN, 1, LANES), F32),
        V((OWN, 8, LANES), F32), V((OWN, 1, LANES), F32),
        V((SIDE, 1, LANES), F32), V((SUB, 1, LANES), F32), V((8, 256), F32),
        V((SIDE, BLK, SUB * BLK), F32), V((SIDE, BLK + TAIL, LANES), F32),
        V((SIDE, BLK, BLK), F32),
        V((SIDE, 2 * SIDE * BLK, 5 * LANES), BF16), V((SIDE, 2 * BLK, BLK), BF16),
        V((SUB, MSG, LANES), F32), V((SUB, HALF, LANES), F32),
        V((2, PACK, SUB * HALF), BF16), V((2, SUB * HALF, PACK), BF16), V((4 * LANES, 256), BF16),
        V((256, 4 * LANES), BF16),
        V((ITERS, VEC, LANES), F32), V((ITERS, SIDE, VEC, LANES), F32),
        V((SIDE, SIDE * BLK, 2 * LANES), BF16), V((8, LANES), F32), V((3, 8, LANES), F32),
        V((SUB, HALF, LANES), F32), V((SUB, MSG, LANES), F32), V((4 * LANES, 256), F32),
        V((PACK, LANES), F32), V((SIDE, BLK, LANES), F32), V((256, 256), F32), V((PACK, LANES), F32),
        V((SIDE, BLK, LANES), F32), V((3, SUB * HALF, LANES), F32),
        dma((5,)),
        dma, dma, dma, dma, dma, dma, dma, dma,
        dma, dma, dma, dma((8,)), dma, dma,
        dma, dma, dma((ITERS,)), dma((2, 7)), dma, dma,
        dma, dma, dma, dma,
    ]
    corr, resid = pl.pallas_call(
        kernel,
        out_shape=(
            jax.ShapeDtypeStruct(residual.shape, F32),
            jax.ShapeDtypeStruct((BLK, 8 * OWN), F32),
        ),
        in_specs=[anywhere] * 5,
        out_specs=(vmem, vmem),
        scratch_shapes=scratch,
        compiler_params=pltpu.CompilerParams(
            collective_id=0, has_side_effects=True, vmem_limit_bytes=62 * 1024 * 1024
        ),
    )(counts, residual, jnp.transpose(assembly[0], (1, 0, 2)), level_two[0], block_inverse[0])
    corr, resid = pl.pallas_call(
        hand_on,
        out_shape=(
            jax.ShapeDtypeStruct(corr.shape, F32), jax.ShapeDtypeStruct(resid.shape, F32)
        ),
        in_specs=[vmem, vmem],
        out_specs=(vmem, vmem),
    )(corr, resid)
    return corr, resid[None]


def solution(mesh):
    in_specs = (
        P("owner", "sub"),
        P("owner", "sub"),
        P("owner", "sub", None, None),
        P("owner", "sub", None),
        P("owner", "sub", None),
    )
    out_specs = (P("owner", "sub"), P("owner", "sub", None))
    return jax.shard_map(shards, mesh=mesh, in_specs=in_specs, out_specs=out_specs, check_vma=False)
```

```python
import jax
import jax.numpy as jnp
from jax import lax
from jax.experimental import pallas as pl
from jax.experimental.pallas import tpu as pltpu
from jax.sharding import PartitionSpec as P

ITERS = 4
F32 = jnp.float32
BF16 = jnp.bfloat16
OWN = 32
SUB = 16
SIDE = 4
BLK = 144
SLOT = 18
PRIM = 36
LANES = 128
HALF = 64
PACK = 2 * BLK
MSG = 40
VEC = PACK + 8
TAIL = 24
CUTS = (0, 72, 144, VEC)


def iota(shape, dim):
    return lax.broadcasted_iota(jnp.int32, shape, dim)


def dot(a, b):
    return jnp.dot(a, b, preferred_element_type=F32)


def dot_nt(a, b):
    return lax.dot_general(a, b, (((1,), (1,)), ((), ())), preferred_element_type=F32)


def split(x):
    hi = x.astype(BF16)
    return hi, (x - hi.astype(F32)).astype(BF16)


def half_swap(x):
    return pltpu.roll(x, HALF, 1)


def low_half(shape):
    return iota(shape, 1) < HALF


def block_transpose(t):
    away = iota((8, LANES), 0) - iota((8, LANES), 1) // 16
    out = t
    for shift in range(1, 8):
        moved = pltpu.roll(pltpu.roll(t, shift, 0), LANES - 16 * shift, 1)
        out = jnp.where((away & 7) == shift, moved, out)
    return out


def kernel(
    cnt_hbm, res_hbm, asm_hbm, mat_hbm, inv_hbm,
    corr_ref, resid_ref,
    cnt_ref, res_ref, asm_ref, inv_ref, inv_out,
    zmain, ztail, zmain_in, ztail_in,
    cmain, ctail, cmain_in, ctail_in,
    offs, offs_in, info,
    rows_in, inv_in, inv_full, stack, mstack,
    vsend, vin, land, land_t, pick, pick_t,
    gsend, gin, wide, ssend, sin,
    psend, pin, back, rbuf, rin, local, partial, by_rows, answers,
    loads,
    zs_m, zr_m, zs_t, zr_t, cs_m, cr_m, cs_t, cr_t,
    os, orr, ms, mr, ivs, ivr, vs, vr, gs, gr, ss, sr, ps, pr, rs, rr,
):
    owner = lax.axis_index("owner")
    sub = lax.axis_index("sub")
    core = lax.rem(owner, 2)
    sx, sy = sub // SIDE, lax.rem(sub, SIDE)
    a = sx * (1 - core) + sy * core
    c = sy * (1 - core) + sx * core

    def at(ra, rc):
        return (4 * ra + rc) * (1 - core) + (4 * rc + ra) * core

    def ring(v, step):
        return lax.rem(v + step + SIDE, SIDE)

    def rcopy(src, dst, ssem, rsem, dev):
        return pltpu.make_async_remote_copy(
            src_ref=src, dst_ref=dst, send_sem=ssem, recv_sem=rsem,
            device_id=dev, device_id_type=pl.DeviceIdType.MESH,
        )

    barrier = pltpu.get_barrier_semaphore()

    def each_owner(act):
        act((owner + OWN // 2) & (OWN - 1))

        @pl.loop(1, OWN // 2)
        def _(i):
            act((owner + (OWN // 2 + i)) & (OWN - 1))
            act((owner + (OWN // 2 - i)) & (OWN - 1))

    def greet(dev):
        pl.semaphore_signal(barrier, inc=1, device_id=dev, device_id_type=pl.DeviceIdType.MESH)

    each_owner(lambda peer: greet((peer, sub)))

    @pl.loop(1, SUB)
    def _(j):
        greet((owner, (sub + j) & (SUB - 1)))

    fetches = [
        pltpu.make_async_copy(res_hbm, res_ref, loads.at[0]),
        pltpu.make_async_copy(asm_hbm, asm_ref, loads.at[1]),
        pltpu.make_async_copy(inv_hbm, inv_ref, loads.at[2]),
        pltpu.make_async_copy(mat_hbm, rows_in.at[c], loads.at[3]),
        pltpu.make_async_copy(cnt_hbm, cnt_ref, loads.at[4]),
    ]
    for fetch in fetches:
        fetch.start()

    lane = iota((8, LANES), 1)
    low = low_half((8, LANES))

    fetches[0].wait()

    def tile(t):
        return res_ref[:, LANES * t:LANES * (t + 1)]

    for k in range(4):
        tails = None
        for j in range(8):
            g = 8 * k + j
            if j == 0:
                main = tile(g + k)
            else:
                main = pltpu.roll(
                    jnp.where(lane >= 16 * j, tile(g + k), tile(g + k + 1)), LANES - 16 * j, 1
                )
            zmain[g] = main
            nxt = tile(g + k + 1)
            tails = nxt if j == 0 else jnp.where(lane // 16 == j, nxt, tails)
        moved = block_transpose(tails)
        for j in range(8):
            ztail[8 * k + j] = moved[j:j + 1, :]

    fetches[2].wait()
    inv_out[0:BLK] = inv_ref[:, 0:LANES]
    inv_out[BLK:] = jnp.zeros((TAIL, LANES), F32)
    for g in range(BLK // TAIL):
        inv_out[BLK:, 16 * g:16 * (g + 1)] = inv_ref[TAIL * g:TAIL * (g + 1), LANES:BLK]

    fetches[1].wait()
    fetches[4].wait()
    col = iota((8, SUB * BLK), 1)
    holder_of = col // BLK
    which = jnp.where(iota((8, SUB * BLK), 0) == 0, col - holder_of * BLK, holder_of)
    which = which.astype(F32).astype(BF16)
    info[...] = jnp.zeros_like(info)
    for j in range(4):
        block = asm_ref[:, j, :].astype(F32).astype(BF16)
        info[:, PRIM * j:PRIM * (j + 1)] = dot_nt(which, block)
    place8 = info[...]
    inside = place8.astype(BF16)
    held = place8[1:2, :].astype(jnp.int32)
    dof = iota((1, 256), 1)
    which_sub = ((dof >= PRIM).astype(jnp.int32) + (dof >= 2 * PRIM).astype(jnp.int32)
                 + (dof >= 3 * PRIM).astype(jnp.int32))
    count = jnp.where(which_sub == 0, cnt_ref[0, 0], jnp.where(
        which_sub == 1, cnt_ref[0, 1], jnp.where(which_sub == 2, cnt_ref[0, 2], cnt_ref[0, 3])))
    live = ((dof - PRIM * which_sub) < count) & (dof < BLK)
    held = jnp.where(live, held, -1)
    hot = (held == iota((SUB, 256), 0)).astype(F32)
    upper = (iota((256, 256), 0) < iota((256, 256), 1)).astype(F32).astype(BF16)
    rank = jnp.sum(hot * dot(hot.astype(BF16), upper), axis=0, keepdims=True).astype(jnp.int32)
    hx, hy = held // SIDE, held & 3
    ha = hx * (1 - core) + hy * core
    hk = hy * (1 - core) + hx * core
    spot = ha * LANES + (hk // 2) * HALF + (hk & 1) * SLOT + rank
    spot = jnp.where(live, spot, -1)
    pick[...] = (iota((4 * LANES, 256), 0) == spot).astype(F32).astype(BF16)
    rows = dot_nt(inside, pick[...])
    for j in range(4):
        offs[j] = rows[0:1, LANES * j:LANES * (j + 1)]

    fetches[3].wait()

    pl.semaphore_wait(barrier, OWN - 1 + SUB - 1)

    def group_of(peer):
        px, py = peer // SIDE, lax.rem(peer, SIDE)
        return px * (1 - core) + py * core, py * (1 - core) + px * core

    @pl.loop(1, SUB)
    def _(j):
        peer = lax.rem(sub + j, SUB)
        pa, _pc = group_of(peer)
        rcopy(offs.at[pa], offs_in.at[sub], os, orr, (owner, peer)).start()

    nextc, prevc, oppc = ring(c, 1), ring(c, -1), ring(c, 2)
    c_right, c_left, c_opp = (owner, at(a, nextc)), (owner, at(a, prevc)), (owner, at(a, oppc))
    half = BLK // 2
    top, bottom = pl.ds(0, half), pl.ds(half, half)
    early, late = pl.ds(half, 40), pl.ds(half + 40, 32)
    cuts = [top, early, bottom, pl.ds(0, 40)] + [
        pl.ds(start + at_row, rows) for start in (0, half)
        for at_row, rows in ((0, 40), (40, 32))] + [late, pl.ds(40, 32)]

    def mat_copy(n, slot, dev):
        piece = rows_in.at[slot, cuts[n]]
        return rcopy(piece, piece, ms, mr.at[n], dev)

    for dev in (c_opp, c_right, c_left):
        rcopy(inv_out, inv_in.at[c], ivs, ivr, dev).start()
    for n in range(2):
        mat_copy(n, c, c_right).start()
        mat_copy(2 + n, c, c_left).start()

    def send_residual(peer):
        rcopy(zmain.at[peer], zmain_in.at[owner], zs_m, zr_m, (peer, sub)).start()
        rcopy(ztail.at[peer], ztail_in.at[owner], zs_t, zr_t, (peer, sub)).start()

    each_owner(send_residual)

    others, peers, three = pl.ds(0, OWN - 1), pl.ds(0, SUB - 1), pl.ds(0, SIDE - 1)
    z_main = rcopy(zmain.at[others], zmain_in.at[others], zs_m, zr_m, c_right)
    z_tail = rcopy(ztail.at[others], ztail_in.at[others], zs_t, zr_t, c_right)
    all_offs = rcopy(offs_in.at[peers], offs_in.at[peers], os, orr, c_right)
    all_inv = rcopy(inv_in.at[three], inv_in.at[three], ivs, ivr, c_right)

    zmain_in[owner] = zmain[owner]
    ztail_in[owner] = ztail[owner]
    offs_in[sub] = offs[a]
    inv_in[c] = inv_out[...]
    vin[:, MSG:HALF, :] = jnp.zeros((SUB, HALF - MSG, LANES), F32)
    back[...] = jnp.zeros_like(back)

    def store_rows(k):
        at_hi = pl.multiple_of(k * BLK, 16)
        at_lo = pl.multiple_of((SIDE + k) * BLK, 16)
        lanes = iota((BLK, LANES), 1)

        @pl.loop(0, SIDE)
        def _(d):
            ra = ring(a, d)

            def window(t, kk):
                start = LANES * t + BLK * (at(ra, kk) - kk)
                first, shift = start // LANES, lax.rem(start, LANES)
                after = jnp.minimum(first + 1, SUB * BLK // LANES - 1)
                one = rows_in[k, :, pl.ds(pl.multiple_of(first * LANES, LANES), LANES)]
                two = rows_in[k, :, pl.ds(pl.multiple_of(after * LANES, LANES), LANES)]
                both = jnp.where(lanes >= shift, one, two)
                return pltpu.roll(both, lax.rem(LANES - shift, LANES), 1)

            for t in range(5):
                ends = [kk for kk in range(SIDE)
                        if BLK * kk < LANES * (t + 1) and BLK * (kk + 1) > LANES * t]
                value = window(t, ends[0])
                if len(ends) > 1:
                    edge = BLK * ends[1] - LANES * t
                    value = jnp.where(lanes < edge, value, window(t, ends[1]))
                hi, lo = split(value)
                cols = slice(LANES * t, LANES * (t + 1))
                stack[d, pl.ds(at_hi, BLK), cols] = hi
                stack[d, pl.ds(at_lo, BLK), cols] = lo

    store_rows(c)

    z_main.wait_recv()
    z_tail.wait_recv()

    local[:, 0:LANES] = zmain_in[...].reshape(8 * OWN, LANES)
    for k in range(4):
        moved = block_transpose(ztail_in[8 * k:8 * (k + 1)].reshape(8, LANES))
        for j in range(8):
            src = 8 * k + j
            local[8 * src:8 * (src + 1), LANES:] = moved if j == 0 else pltpu.roll(
                moved, LANES - 16 * j, 1)
    loc_hi, loc_lo = split(local[...])
    vals = dot_nt(pick[...], loc_hi) + dot_nt(pick[...], loc_lo)
    low_msg = low_half((MSG, LANES))
    for ra in range(4):
        for t in range(2):
            first = vals[LANES * ra:LANES * ra + MSG, LANES * t:LANES * (t + 1)]
            second = vals[LANES * ra + HALF:LANES * ra + HALF + MSG, LANES * t:LANES * (t + 1)]
            vsend[4 * ra + 2 * t] = jnp.where(low_msg, first, half_swap(second))
            vsend[4 * ra + 2 * t + 1] = jnp.where(low_msg, half_swap(first), second)
    body = pl.ds(0, MSG)

    far = sorted(((da, dc) for da in range(4) for dc in range(4) if da or dc),
                 key=lambda d: -(min(d[0], 4 - d[0]) + min(d[1], 4 - d[1])))
    for da, dc in far:
        pa, pc = ring(a, da), ring(c, dc)
        rcopy(vsend.at[4 * pa + pc], vin.at[sub, body], vs, vr, (owner, at(pa, pc))).start()
    mat_copy(8, c, c_right).start()
    mat_copy(9, c, c_left).start()
    all_vals = rcopy(vin.at[peers, body], vin.at[peers, body], vs, vr, c_right)

    vin[sub, body] = vsend[4 * a + c]

    all_offs.wait_recv()

    pick_t[...] = pick[...].astype(F32).T.astype(BF16)

    lane1 = iota((1, LANES), 1)
    extra = jnp.where((lane1 & (HALF - 1)) >= SLOT, float(BLK), 0.0)
    for m in range(SUB // 2):
        one, two = offs_in[2 * m], offs_in[2 * m + 1]
        for h in range(2):
            if h == 0:
                row = jnp.where(lane1 < HALF, one, half_swap(two)) + extra
            else:
                row = jnp.where(lane1 < HALF, half_swap(one), two) + extra
            rowi = row.astype(jnp.int32)
            cols = pl.ds(LANES * m, LANES)
            land[h, :, cols] = (iota((PACK, LANES), 0) == rowi).astype(F32).astype(BF16)
            down = jnp.broadcast_to(row, (LANES, LANES)).T.astype(jnp.int32)
            for t, width in ((0, LANES), (1, LANES), (2, PACK - 2 * LANES)):
                hit = (down == iota((LANES, LANES), 1) + LANES * t).astype(F32).astype(BF16)
                land_t[h, cols, LANES * t:LANES * t + width] = hit[:, :width]

    mat_copy(0, prevc, c_left).wait_recv()
    mat_copy(4, prevc, c_right).start()
    mat_copy(2, nextc, c_right).wait_recv()
    mat_copy(6, nextc, c_left).start()


    all_inv.wait_recv()
    for k in range(4):
        inv_full[k, :, 0:LANES] = inv_in[k, 0:BLK]
        for g in range(BLK // TAIL):
            inv_full[k, TAIL * g:TAIL * (g + 1), LANES:BLK] = inv_in[
                k, BLK:, 16 * g:16 * (g + 1)]
        hi, lo = split(inv_full[k])
        mstack[k, 0:BLK] = hi
        mstack[k, BLK:] = lo

    all_vals.wait_recv()

    low_pack = low_half((PACK, LANES))
    low_blk = low_half((BLK, LANES))

    def side_by_side(x):
        hi, lo = split(x)
        return jnp.concatenate([hi, lo], axis=1)

    def fold(x):
        return x[:, :LANES] + x[:, LANES:]

    values = side_by_side(vin[...].reshape(SUB * HALF, LANES))
    r = jnp.where(low_pack, fold(dot(land[0], values)), fold(dot(land[1], values)))

    def spread(x):
        keep = low_half(x.shape)
        hi = x.astype(BF16).astype(F32)
        rem = x - hi
        mid = rem.astype(BF16).astype(F32)
        lo = rem - mid
        mid_ = half_swap(mid)
        first = (jnp.where(keep, hi, mid_), jnp.where(keep, lo, 0.0))
        second = (jnp.where(keep, mid_, hi), jnp.where(keep, 0.0, lo))
        return tuple(jnp.concatenate(p, axis=1).astype(BF16) for p in (first, second))

    def gathered(x):
        one = x[:, :LANES] + x[:, LANES:]
        return one + half_swap(one)

    def precond_half(parts, kk):
        done = []
        for k in (kk, 2 + kk):
            got = dot(mstack[k], parts[k // 2][kk * BLK:(kk + 1) * BLK])
            done.append(gathered(got[:BLK] + got[BLK:]))
        return jnp.where(low_blk, done[0], done[1])

    nexta, preva, oppa = ring(a, 1), ring(a, -1), ring(a, 2)
    a_right, a_left, a_opp = (owner, at(nexta, c)), (owner, at(preva, c)), (owner, at(oppa, c))
    head, tail, after = (pl.ds(CUTS[i], CUTS[i + 1] - CUTS[i]) for i in range(3))
    parts_of = [head, pl.ds(CUTS[1], VEC - CUTS[1]), tail, head, after, head, tail, after]
    toward = [a_right, a_right, a_left, a_left, a_opp, a_right, a_left, a_left]

    def vec_copy(it, n, slot):
        part = parts_of[n]
        source = gin.at[it, slot, part] if n in (5, 6) else gsend.at[it, part]
        return rcopy(source, gin.at[it, slot, part], gs.at[it], gr.at[it % 2, n], toward[n])

    def widen(d, x):
        first, second = spread(x)
        wide[d, 0:PACK] = first
        wide[d, PACK:] = second

    def product(d):
        out = []
        for h in range(2):
            got = dot(stack[d, PACK * h:PACK * (h + 1), 0:2 * PACK], wide[d])
            got = got + dot(stack[d, PACK * (2 + h):PACK * (3 + h), 0:2 * PACK], wide[d])
            out.append(gathered(got))
        return jnp.where(low_pack, out[0], out[1])

    def product_rows(k, chunks):
        got = None
        for d in chunks:
            for first in (k, SIDE + k):
                rows = stack[d, pl.ds(pl.multiple_of(first * BLK, 16), BLK), 0:2 * PACK]
                term = dot(rows, wide[d])
                got = term if got is None else got + term
        got = gathered(got)
        by_rows[k] = got if chunks[0] == 0 else by_rows[k] + got

    def gather_start(it, v, sums_of):
        parts = spread(v)
        first = precond_half(parts, 0)
        gsend[it, 0:BLK] = first
        for n in (0, 2):
            vec_copy(it, n, a).start()
        sums = sums_of()
        second = precond_half(parts, 1)
        gsend[it, BLK:PACK] = second
        gsend[it, PACK:VEC] = sums
        for n in (1, 3, 7, 4):
            vec_copy(it, n, a).start()
        out = jnp.concatenate([first, second], axis=0)
        widen(0, out)
        return out, sums

    def gather_pass(it):
        vec_copy(it, 0, preva).wait_recv()
        vec_copy(it, 5, preva).start()
        vec_copy(it, 2, nexta).wait_recv()
        vec_copy(it, 6, nexta).start()

    def gather_near(it):
        vec_copy(it, 1, preva).wait_recv()
        widen(3, gin[it, preva, 0:PACK])
        vec_copy(it, 3, nexta).wait_recv()
        vec_copy(it, 7, nexta).wait_recv()
        widen(1, gin[it, nexta, 0:PACK])

    def gather_end(it, sums):
        for n in (4, 5, 6):
            vec_copy(it, n, oppa).wait_recv()
        widen(2, gin[it, oppa, 0:PACK])
        total = sums
        for ra in (preva, nexta, oppa):
            total = total + gin[it, ra, PACK:VEC]
        return total

    def column_sum(x, y):
        s = jnp.sum(x * y, axis=0, keepdims=True)
        return s + half_swap(s)

    row8 = iota((8, LANES), 0)

    def partial_sums(r, u, w):
        one, two = column_sum(r, u), column_sum(w, u)
        return jnp.where(row8 == 0, one, jnp.where(row8 == 1, two, 0.0))

    nothing = jnp.zeros((8, LANES), F32)
    u, _ = gather_start(0, r, lambda: nothing)
    mat_copy(5, prevc, c_right).start()
    mat_copy(7, nextc, c_left).start()
    mat_copy(1, prevc, c_left).wait_recv()
    mat_copy(8, prevc, c_left).wait_recv()
    store_rows(prevc)
    mat_copy(3, nextc, c_right).wait_recv()
    mat_copy(9, nextc, c_right).wait_recv()
    store_rows(nextc)

    gather_pass(0)
    for k in (c, prevc, nextc):
        product_rows(k, (0,))
    gather_near(0)
    for k in (c, prevc, nextc):
        product_rows(k, (1, 3))
    gather_end(0, nothing)
    for k in (c, prevc, nextc):
        product_rows(k, (2,))
    for n in range(4, 8):
        mat_copy(n, oppc, c_right).wait_recv()
    store_rows(oppc)
    product_rows(oppc, (0, 1, 3, 2))
    w = jnp.concatenate(
        [jnp.where(low_blk, by_rows[kk], by_rows[2 + kk]) for kk in range(2)], axis=0)

    gamma = alpha = None
    x = p = s = q = z = None
    for it in range(1, ITERS):
        m, sums = gather_start(it, w, lambda: partial_sums(r, u, w))
        partial[...] = product(0)
        gather_pass(it)
        gather_near(it)
        partial[...] = partial[...] + product(1) + product(3)
        total = gather_end(it, sums)
        n = partial[...] + product(2)
        gamma_new, delta = total[0:1], total[1:2]
        if it == 1:
            alpha = gamma_new / delta
            z, q, s, p = n, m, w, u
            x = alpha * p
        else:
            beta = gamma_new / gamma
            alpha = gamma_new / (delta - beta * gamma_new / alpha)
            z, q, s, p = n + beta * z, m + beta * q, w + beta * s, u + beta * p
            x = x + alpha * p
        gamma = gamma_new
        r = r - alpha * s
        u = u - alpha * q
        w = w - alpha * z

    sums = partial_sums(r, u, w)
    ssend[...] = sums
    for n, dev in ((2, a_opp), (0, a_right), (1, a_left)):
        rcopy(ssend, sin.at[n], ss, sr, dev).start()
    all_sums = rcopy(sin, sin, ss, sr, a_right)

    low_slots = low_half((SUB * HALF, LANES))

    def reply_of(v):
        vs_ = side_by_side(v)
        return jnp.where(low_slots, fold(dot(land_t[0], vs_)), fold(dot(land_t[1], vs_)))

    for n, v in ((0, x), (1, u), (2, p)):
        answers[n] = reply_of(v)
    all_sums.wait_recv()
    total = sums + sin[0] + sin[1] + sin[2]
    gamma_new, delta = total[0:1], total[1:2]
    beta = gamma_new / gamma
    alpha = gamma_new / (delta - beta * gamma_new / alpha)
    reply = answers[0] + alpha * (answers[1] + beta * answers[2])
    psend[...] = reply.reshape(SUB, HALF, LANES)
    mine = 4 * a + c

    for da, dc in far:
        peer = at(ring(a, da), ring(c, dc))
        rcopy(psend.at[peer, body], pin.at[mine], ps, pr, (owner, peer)).start()
    all_back = rcopy(pin.at[peers], pin.at[peers], ps, pr, c_right)

    pin[mine] = psend[sub, body]

    rbuf[...] = r - alpha * (w + beta * s)
    for slot, dev in ((oppc, c_opp), (nextc, c_right), (prevc, c_left)):
        source = rbuf.at[pl.ds(pl.multiple_of(lax.rem(slot, 2) * BLK, 8), BLK)]
        rcopy(source, rin.at[c], rs, rr, dev).start()
    all_resid = rcopy(rin.at[three], rin.at[three], rs, rr, c_right)
    rin[c] = rbuf[pl.ds(pl.multiple_of(lax.rem(c, 2) * BLK, 8), BLK)]

    all_back.wait_recv()

    for ra in range(4):
        for t in range(2):
            one, two = pin[4 * ra + 2 * t], pin[4 * ra + 2 * t + 1]
            cols = slice(LANES * t, LANES * (t + 1))
            back[LANES * ra:LANES * ra + MSG, cols] = jnp.where(low_msg, one, half_swap(two))
            back[LANES * ra + HALF:LANES * ra + HALF + MSG, cols] = jnp.where(
                low_msg, half_swap(one), two)
    back_hi, back_lo = split(back[...])
    mine_back = (dot(pick_t[...], back_hi) + dot(pick_t[...], back_lo)).T
    cmain[...] = mine_back[:, :LANES].reshape(OWN, 8, LANES)
    for k in range(4):
        tails = None
        for j in range(8):
            src = 8 * k + j
            piece = mine_back[8 * src:8 * (src + 1), LANES:]
            tails = piece if j == 0 else tails + pltpu.roll(piece, 16 * j, 1)
        moved = block_transpose(tails)
        for j in range(8):
            ctail[8 * k + j] = moved[j:j + 1, :]

    def send_correction(peer):
        rcopy(cmain.at[peer], cmain_in.at[owner], cs_m, cr_m, (peer, sub)).start()
        rcopy(ctail.at[peer], ctail_in.at[owner], cs_t, cr_t, (peer, sub)).start()

    each_owner(send_correction)

    c_main = rcopy(cmain.at[others], cmain_in.at[others], cs_m, cr_m, c_right)
    c_tail = rcopy(ctail.at[others], ctail_in.at[others], cs_t, cr_t, c_right)

    cmain_in[owner] = cmain[owner]
    ctail_in[owner] = ctail[owner]

    all_resid.wait_recv()
    for t in range(2):
        one, two = rin[2 * t], rin[2 * t + 1]
        upper_half = jnp.where(low_blk, half_swap(one), two)
        lower_half = jnp.where(low_blk, one, half_swap(two))
        resid_ref[:, LANES * t:LANES * (t + 1)] = jnp.where(c < 2, lower_half, upper_half)

    rcopy(rows_in.at[three], rows_in.at[three], ms, mr.at[0], c_right).wait_send()
    for it in range(ITERS):
        rcopy(gin.at[it, three], gin.at[it, three], gs.at[it], gr.at[0, 0], c_right).wait_send()
    for sent in (z_main, z_tail, all_offs, all_inv, all_vals, all_sums, all_back, all_resid):
        sent.wait_send()
    c_main.wait_recv()
    c_tail.wait_recv()
    c_main.wait_send()
    c_tail.wait_send()

    for k in range(4):
        tails = block_transpose(ctail_in[8 * k:8 * (k + 1)].reshape(8, LANES))
        turned = [
            cmain_in[8 * k + j] if j == 0 else pltpu.roll(cmain_in[8 * k + j], 16 * j, 1)
            for j in range(8)
        ]
        for m in range(9):
            if m == 0:
                value = turned[0]
            else:
                value = jnp.where(lane < 16 * m, tails, turned[m]) if m < 8 else tails
                value = jnp.where(lane < 16 * (m - 1), turned[m - 1], value)
            where_to = LANES * (9 * k + m)
            corr_ref[:, where_to:where_to + LANES] = value


def hand_on(corr_in, resid_in, corr_out, resid_out):
    corr_out[...] = corr_in[...]
    resid_out[...] = resid_in[...]


def shards(residual, counts, assembly, level_two, block_inverse):
    vmem = pl.BlockSpec(memory_space=pltpu.VMEM)
    anywhere = pl.BlockSpec(memory_space=pl.ANY)
    V = pltpu.VMEM
    dma = pltpu.SemaphoreType.DMA
    scratch = [
        pltpu.SMEM(counts.shape, jnp.int32),
        V(residual.shape, F32), V((PRIM, SIDE, SUB * BLK), jnp.int32), V((BLK, BLK), F32),
        V((BLK + TAIL, LANES), F32),
        V((OWN, 8, LANES), F32), V((OWN, 1, LANES), F32),
        V((OWN, 8, LANES), F32), V((OWN, 1, LANES), F32),
        V((OWN, 8, LANES), F32), V((OWN, 1, LANES), F32),
        V((OWN, 8, LANES), F32), V((OWN, 1, LANES), F32),
        V((SIDE, 1, LANES), F32), V((SUB, 1, LANES), F32), V((8, 256), F32),
        V((SIDE, BLK, SUB * BLK), F32), V((SIDE, BLK + TAIL, LANES), F32),
        V((SIDE, BLK, BLK), F32),
        V((SIDE, 2 * SIDE * BLK, 5 * LANES), BF16), V((SIDE, 2 * BLK, BLK), BF16),
        V((SUB, MSG, LANES), F32), V((SUB, HALF, LANES), F32),
        V((2, PACK, SUB * HALF), BF16), V((2, SUB * HALF, PACK), BF16), V((4 * LANES, 256), BF16),
        V((256, 4 * LANES), BF16),
        V((ITERS, VEC, LANES), F32), V((ITERS, SIDE, VEC, LANES), F32),
        V((SIDE, SIDE * BLK, 2 * LANES), BF16), V((8, LANES), F32), V((3, 8, LANES), F32),
        V((SUB, HALF, LANES), F32), V((SUB, MSG, LANES), F32), V((4 * LANES, 256), F32),
        V((PACK, LANES), F32), V((SIDE, BLK, LANES), F32), V((256, 256), F32), V((PACK, LANES), F32),
        V((SIDE, BLK, LANES), F32), V((3, SUB * HALF, LANES), F32),
        dma((5,)),
        dma, dma, dma, dma, dma, dma, dma, dma,
        dma, dma, dma, dma((10,)), dma, dma,
        dma, dma, dma((ITERS,)), dma((2, 8)), dma, dma,
        dma, dma, dma, dma,
    ]
    corr, resid = pl.pallas_call(
        kernel,
        out_shape=(
            jax.ShapeDtypeStruct(residual.shape, F32),
            jax.ShapeDtypeStruct((BLK, 8 * OWN), F32),
        ),
        in_specs=[anywhere] * 5,
        out_specs=(vmem, vmem),
        scratch_shapes=scratch,
        compiler_params=pltpu.CompilerParams(
            collective_id=0, has_side_effects=True, vmem_limit_bytes=62 * 1024 * 1024
        ),
    )(counts, residual, jnp.transpose(assembly[0], (1, 0, 2)), level_two[0], block_inverse[0])
    corr, resid = pl.pallas_call(
        hand_on,
        out_shape=(
            jax.ShapeDtypeStruct(corr.shape, F32), jax.ShapeDtypeStruct(resid.shape, F32)
        ),
        in_specs=[vmem, vmem],
        out_specs=(vmem, vmem),
    )(corr, resid)
    return corr, resid[None]


def solution(mesh):
    in_specs = (
        P("owner", "sub"),
        P("owner", "sub"),
        P("owner", "sub", None, None),
        P("owner", "sub", None),
        P("owner", "sub", None),
    )
    out_specs = (P("owner", "sub"), P("owner", "sub", None))
    return jax.shard_map(shards, mesh=mesh, in_specs=in_specs, out_specs=out_specs, check_vma=False)
```

```python
import jax
import jax.numpy as jnp
from jax import lax
from jax.experimental import pallas as pl
from jax.experimental.pallas import tpu as pltpu
from jax.sharding import PartitionSpec as P

ITERS = 4
F32 = jnp.float32
BF16 = jnp.bfloat16
OWN = 32
SUB = 16
SIDE = 4
BLK = 144
SLOT = 18
PRIM = 36
LANES = 128
HALF = 64
PACK = 2 * BLK
MSG = 40
VEC = PACK + 8
TAIL = 24
CUTS = (0, 72, 144, VEC)


def iota(shape, dim):
    return lax.broadcasted_iota(jnp.int32, shape, dim)


def dot(a, b):
    return jnp.dot(a, b, preferred_element_type=F32)


def dot_nt(a, b):
    return lax.dot_general(a, b, (((1,), (1,)), ((), ())), preferred_element_type=F32)


def split(x):
    hi = x.astype(BF16)
    return hi, (x - hi.astype(F32)).astype(BF16)


def half_swap(x):
    return pltpu.roll(x, HALF, 1)


def low_half(shape):
    return iota(shape, 1) < HALF


def block_transpose(t):
    away = iota((8, LANES), 0) - iota((8, LANES), 1) // 16
    out = t
    for shift in range(1, 8):
        moved = pltpu.roll(pltpu.roll(t, shift, 0), LANES - 16 * shift, 1)
        out = jnp.where((away & 7) == shift, moved, out)
    return out


def kernel(
    cnt_hbm, res_hbm, asm_hbm, mat_hbm, inv_hbm,
    corr_ref, resid_ref,
    cnt_ref, res_ref, asm_ref, inv_ref, inv_out,
    zmain, ztail, zmain_in, ztail_in,
    cmain, ctail, cmain_in, ctail_in,
    offs, offs_in, info,
    rows_in, inv_in, inv_full, stack, mstack,
    vsend, vin, land, land_t, pick, pick_t,
    gsend, gin, wide, ssend, sin,
    psend, pin, back, rbuf, rin, local, partial, by_rows, answers,
    loads,
    zs_m, zr_m, zs_t, zr_t, cs_m, cr_m, cs_t, cr_t,
    os, orr, ms, mr, ivs, ivr, vs, vr, gs, gr, ss, sr, ps, pr, rs, rr,
):
    owner = lax.axis_index("owner")
    sub = lax.axis_index("sub")
    core = lax.rem(owner, 2)
    sx, sy = sub // SIDE, lax.rem(sub, SIDE)
    a = sx * (1 - core) + sy * core
    c = sy * (1 - core) + sx * core

    def at(ra, rc):
        return (4 * ra + rc) * (1 - core) + (4 * rc + ra) * core

    def ring(v, step):
        return lax.rem(v + step + SIDE, SIDE)

    def rcopy(src, dst, ssem, rsem, dev):
        return pltpu.make_async_remote_copy(
            src_ref=src, dst_ref=dst, send_sem=ssem, recv_sem=rsem,
            device_id=dev, device_id_type=pl.DeviceIdType.MESH,
        )

    barrier = pltpu.get_barrier_semaphore()

    def each_owner(act):
        act((owner + OWN // 2) & (OWN - 1))

        @pl.loop(1, OWN // 2)
        def _(i):
            act((owner + (OWN // 2 + i)) & (OWN - 1))
            act((owner + (OWN // 2 - i)) & (OWN - 1))

    def greet(dev):
        pl.semaphore_signal(barrier, inc=1, device_id=dev, device_id_type=pl.DeviceIdType.MESH)

    each_owner(lambda peer: greet((peer, sub)))

    @pl.loop(1, SUB)
    def _(j):
        greet((owner, (sub + j) & (SUB - 1)))

    fetches = [
        pltpu.make_async_copy(res_hbm, res_ref, loads.at[0]),
        pltpu.make_async_copy(asm_hbm, asm_ref, loads.at[1]),
        pltpu.make_async_copy(inv_hbm, inv_ref, loads.at[2]),
        pltpu.make_async_copy(mat_hbm, rows_in.at[c], loads.at[3]),
        pltpu.make_async_copy(cnt_hbm, cnt_ref, loads.at[4]),
    ]
    for fetch in fetches:
        fetch.start()

    lane = iota((8, LANES), 1)
    low = low_half((8, LANES))

    fetches[0].wait()

    def tile(t):
        return res_ref[:, LANES * t:LANES * (t + 1)]

    for k in range(4):
        tails = None
        for j in range(8):
            g = 8 * k + j
            if j == 0:
                main = tile(g + k)
            else:
                main = pltpu.roll(
                    jnp.where(lane >= 16 * j, tile(g + k), tile(g + k + 1)), LANES - 16 * j, 1
                )
            zmain[g] = main
            nxt = tile(g + k + 1)
            tails = nxt if j == 0 else jnp.where(lane // 16 == j, nxt, tails)
        moved = block_transpose(tails)
        for j in range(8):
            ztail[8 * k + j] = moved[j:j + 1, :]

    fetches[2].wait()
    inv_out[0:BLK] = inv_ref[:, 0:LANES]
    inv_out[BLK:] = jnp.zeros((TAIL, LANES), F32)
    for g in range(BLK // TAIL):
        inv_out[BLK:, 16 * g:16 * (g + 1)] = inv_ref[TAIL * g:TAIL * (g + 1), LANES:BLK]

    fetches[1].wait()
    fetches[4].wait()
    col = iota((8, SUB * BLK), 1)
    holder_of = col // BLK
    which = jnp.where(iota((8, SUB * BLK), 0) == 0, col - holder_of * BLK, holder_of)
    which = which.astype(F32).astype(BF16)
    info[...] = jnp.zeros_like(info)
    for j in range(4):
        block = asm_ref[:, j, :].astype(F32).astype(BF16)
        info[:, PRIM * j:PRIM * (j + 1)] = dot_nt(which, block)
    place8 = info[...]
    inside = place8.astype(BF16)
    held = place8[1:2, :].astype(jnp.int32)
    dof = iota((1, 256), 1)
    which_sub = ((dof >= PRIM).astype(jnp.int32) + (dof >= 2 * PRIM).astype(jnp.int32)
                 + (dof >= 3 * PRIM).astype(jnp.int32))
    count = jnp.where(which_sub == 0, cnt_ref[0, 0], jnp.where(
        which_sub == 1, cnt_ref[0, 1], jnp.where(which_sub == 2, cnt_ref[0, 2], cnt_ref[0, 3])))
    live = ((dof - PRIM * which_sub) < count) & (dof < BLK)
    held = jnp.where(live, held, -1)
    hot = (held == iota((SUB, 256), 0)).astype(F32)
    upper = (iota((256, 256), 0) < iota((256, 256), 1)).astype(F32).astype(BF16)
    rank = jnp.sum(hot * dot(hot.astype(BF16), upper), axis=0, keepdims=True).astype(jnp.int32)
    hx, hy = held // SIDE, held & 3
    ha = hx * (1 - core) + hy * core
    hk = hy * (1 - core) + hx * core
    spot = ha * LANES + (hk // 2) * HALF + (hk & 1) * SLOT + rank
    spot = jnp.where(live, spot, -1)
    pick[...] = (iota((4 * LANES, 256), 0) == spot).astype(F32).astype(BF16)
    rows = dot_nt(inside, pick[...])
    for j in range(4):
        offs[j] = rows[0:1, LANES * j:LANES * (j + 1)]

    fetches[3].wait()

    pl.semaphore_wait(barrier, OWN - 1 + SUB - 1)

    def group_of(peer):
        px, py = peer // SIDE, lax.rem(peer, SIDE)
        return px * (1 - core) + py * core, py * (1 - core) + px * core

    @pl.loop(1, SUB)
    def _(j):
        peer = lax.rem(sub + j, SUB)
        pa, _pc = group_of(peer)
        rcopy(offs.at[pa], offs_in.at[sub], os, orr, (owner, peer)).start()

    nextc, prevc, oppc = ring(c, 1), ring(c, -1), ring(c, 2)
    c_right, c_left, c_opp = (owner, at(a, nextc)), (owner, at(a, prevc)), (owner, at(a, oppc))
    half = BLK // 2
    top, bottom = pl.ds(0, half), pl.ds(half, half)
    early, late = pl.ds(half, 40), pl.ds(half + 40, 32)
    cuts = [top, early, bottom, pl.ds(0, 40)] + [
        pl.ds(start + at_row, rows) for start in (0, half)
        for at_row, rows in ((0, 40), (40, 32))] + [late, pl.ds(40, 32)]

    def mat_copy(n, slot, dev):
        piece = rows_in.at[slot, cuts[n]]
        return rcopy(piece, piece, ms, mr.at[n], dev)

    mat_copy(0, c, c_right).start()
    mat_copy(2, c, c_left).start()
    for dev in (c_opp, c_right, c_left):
        rcopy(inv_out, inv_in.at[c], ivs, ivr, dev).start()
    mat_copy(1, c, c_right).start()
    mat_copy(3, c, c_left).start()

    def send_residual(peer):
        rcopy(zmain.at[peer], zmain_in.at[owner], zs_m, zr_m, (peer, sub)).start()
        rcopy(ztail.at[peer], ztail_in.at[owner], zs_t, zr_t, (peer, sub)).start()

    each_owner(send_residual)

    others, peers, three = pl.ds(0, OWN - 1), pl.ds(0, SUB - 1), pl.ds(0, SIDE - 1)
    z_main = rcopy(zmain.at[others], zmain_in.at[others], zs_m, zr_m, c_right)
    z_tail = rcopy(ztail.at[others], ztail_in.at[others], zs_t, zr_t, c_right)
    all_offs = rcopy(offs_in.at[peers], offs_in.at[peers], os, orr, c_right)
    all_inv = rcopy(inv_in.at[three], inv_in.at[three], ivs, ivr, c_right)

    zmain_in[owner] = zmain[owner]
    ztail_in[owner] = ztail[owner]
    offs_in[sub] = offs[a]
    inv_in[c] = inv_out[...]
    vin[:, MSG:HALF, :] = jnp.zeros((SUB, HALF - MSG, LANES), F32)
    back[...] = jnp.zeros_like(back)

    def store_rows(k):
        at_hi = pl.multiple_of(k * BLK, 16)
        at_lo = pl.multiple_of((SIDE + k) * BLK, 16)
        lanes = iota((BLK, LANES), 1)

        @pl.loop(0, SIDE)
        def _(d):
            ra = ring(a, d)

            def window(t, kk):
                start = LANES * t + BLK * (at(ra, kk) - kk)
                first, shift = start // LANES, lax.rem(start, LANES)
                after = jnp.minimum(first + 1, SUB * BLK // LANES - 1)
                one = rows_in[k, :, pl.ds(pl.multiple_of(first * LANES, LANES), LANES)]
                two = rows_in[k, :, pl.ds(pl.multiple_of(after * LANES, LANES), LANES)]
                both = jnp.where(lanes >= shift, one, two)
                return pltpu.roll(both, lax.rem(LANES - shift, LANES), 1)

            for t in range(5):
                ends = [kk for kk in range(SIDE)
                        if BLK * kk < LANES * (t + 1) and BLK * (kk + 1) > LANES * t]
                value = window(t, ends[0])
                if len(ends) > 1:
                    edge = BLK * ends[1] - LANES * t
                    value = jnp.where(lanes < edge, value, window(t, ends[1]))
                hi, lo = split(value)
                cols = slice(LANES * t, LANES * (t + 1))
                stack[d, pl.ds(at_hi, BLK), cols] = hi
                stack[d, pl.ds(at_lo, BLK), cols] = lo

    store_rows(c)

    z_main.wait_recv()
    z_tail.wait_recv()

    local[:, 0:LANES] = zmain_in[...].reshape(8 * OWN, LANES)
    for k in range(4):
        moved = block_transpose(ztail_in[8 * k:8 * (k + 1)].reshape(8, LANES))
        for j in range(8):
            src = 8 * k + j
            local[8 * src:8 * (src + 1), LANES:] = moved if j == 0 else pltpu.roll(
                moved, LANES - 16 * j, 1)
    loc_hi, loc_lo = split(local[...])
    vals = dot_nt(pick[...], loc_hi) + dot_nt(pick[...], loc_lo)
    low_msg = low_half((MSG, LANES))
    for ra in range(4):
        for t in range(2):
            first = vals[LANES * ra:LANES * ra + MSG, LANES * t:LANES * (t + 1)]
            second = vals[LANES * ra + HALF:LANES * ra + HALF + MSG, LANES * t:LANES * (t + 1)]
            vsend[4 * ra + 2 * t] = jnp.where(low_msg, first, half_swap(second))
            vsend[4 * ra + 2 * t + 1] = jnp.where(low_msg, half_swap(first), second)
    body = pl.ds(0, MSG)

    far = sorted(((da, dc) for da in range(4) for dc in range(4) if da or dc),
                 key=lambda d: -(min(d[0], 4 - d[0]) + min(d[1], 4 - d[1])))
    for da, dc in far:
        pa, pc = ring(a, da), ring(c, dc)
        rcopy(vsend.at[4 * pa + pc], vin.at[sub, body], vs, vr, (owner, at(pa, pc))).start()
    mat_copy(8, c, c_right).start()
    mat_copy(9, c, c_left).start()
    all_vals = rcopy(vin.at[peers, body], vin.at[peers, body], vs, vr, c_right)

    vin[sub, body] = vsend[4 * a + c]

    all_offs.wait_recv()

    pick_t[...] = pick[...].astype(F32).T.astype(BF16)

    lane1 = iota((1, LANES), 1)
    extra = jnp.where((lane1 & (HALF - 1)) >= SLOT, float(BLK), 0.0)
    for m in range(SUB // 2):
        one, two = offs_in[2 * m], offs_in[2 * m + 1]
        for h in range(2):
            if h == 0:
                row = jnp.where(lane1 < HALF, one, half_swap(two)) + extra
            else:
                row = jnp.where(lane1 < HALF, half_swap(one), two) + extra
            rowi = row.astype(jnp.int32)
            cols = pl.ds(LANES * m, LANES)
            land[h, :, cols] = (iota((PACK, LANES), 0) == rowi).astype(F32).astype(BF16)
            down = jnp.broadcast_to(row, (LANES, LANES)).T.astype(jnp.int32)
            for t, width in ((0, LANES), (1, LANES), (2, PACK - 2 * LANES)):
                hit = (down == iota((LANES, LANES), 1) + LANES * t).astype(F32).astype(BF16)
                land_t[h, cols, LANES * t:LANES * t + width] = hit[:, :width]

    mat_copy(0, prevc, c_left).wait_recv()
    mat_copy(4, prevc, c_right).start()
    mat_copy(2, nextc, c_right).wait_recv()
    mat_copy(6, nextc, c_left).start()


    all_inv.wait_recv()
    for k in range(4):
        inv_full[k, :, 0:LANES] = inv_in[k, 0:BLK]
        for g in range(BLK // TAIL):
            inv_full[k, TAIL * g:TAIL * (g + 1), LANES:BLK] = inv_in[
                k, BLK:, 16 * g:16 * (g + 1)]
        hi, lo = split(inv_full[k])
        mstack[k, 0:BLK] = hi
        mstack[k, BLK:] = lo

    all_vals.wait_recv()

    low_pack = low_half((PACK, LANES))
    low_blk = low_half((BLK, LANES))

    def side_by_side(x):
        hi, lo = split(x)
        return jnp.concatenate([hi, lo], axis=1)

    def fold(x):
        return x[:, :LANES] + x[:, LANES:]

    values = side_by_side(vin[...].reshape(SUB * HALF, LANES))
    r = jnp.where(low_pack, fold(dot(land[0], values)), fold(dot(land[1], values)))

    def spread(x):
        keep = low_half(x.shape)
        hi = x.astype(BF16).astype(F32)
        rem = x - hi
        mid = rem.astype(BF16).astype(F32)
        lo = rem - mid
        mid_ = half_swap(mid)
        first = (jnp.where(keep, hi, mid_), jnp.where(keep, lo, 0.0))
        second = (jnp.where(keep, mid_, hi), jnp.where(keep, 0.0, lo))
        return tuple(jnp.concatenate(p, axis=1).astype(BF16) for p in (first, second))

    def gathered(x):
        one = x[:, :LANES] + x[:, LANES:]
        return one + half_swap(one)

    def precond_half(parts, kk):
        done = []
        for k in (kk, 2 + kk):
            got = dot(mstack[k], parts[k // 2][kk * BLK:(kk + 1) * BLK])
            done.append(gathered(got[:BLK] + got[BLK:]))
        return jnp.where(low_blk, done[0], done[1])

    nexta, preva, oppa = ring(a, 1), ring(a, -1), ring(a, 2)
    a_right, a_left, a_opp = (owner, at(nexta, c)), (owner, at(preva, c)), (owner, at(oppa, c))
    head, tail, after = (pl.ds(CUTS[i], CUTS[i + 1] - CUTS[i]) for i in range(3))
    parts_of = [head, pl.ds(CUTS[1], VEC - CUTS[1]), tail, head, after, head, tail, after]
    toward = [a_right, a_right, a_left, a_left, a_opp, a_right, a_left, a_left]

    def vec_copy(it, n, slot):
        part = parts_of[n]
        source = gin.at[it, slot, part] if n in (5, 6) else gsend.at[it, part]
        return rcopy(source, gin.at[it, slot, part], gs.at[it], gr.at[it % 2, n], toward[n])

    def widen(d, x):
        first, second = spread(x)
        wide[d, 0:PACK] = first
        wide[d, PACK:] = second

    def product(d):
        out = []
        for h in range(2):
            got = dot(stack[d, PACK * h:PACK * (h + 1), 0:2 * PACK], wide[d])
            got = got + dot(stack[d, PACK * (2 + h):PACK * (3 + h), 0:2 * PACK], wide[d])
            out.append(gathered(got))
        return jnp.where(low_pack, out[0], out[1])

    def product_rows(k, chunks):
        got = None
        for d in chunks:
            for first in (k, SIDE + k):
                rows = stack[d, pl.ds(pl.multiple_of(first * BLK, 16), BLK), 0:2 * PACK]
                term = dot(rows, wide[d])
                got = term if got is None else got + term
        got = gathered(got)
        by_rows[k] = got if chunks[0] == 0 else by_rows[k] + got

    def gather_start(it, v, sums_of):
        parts = spread(v)
        first = precond_half(parts, 0)
        gsend[it, 0:BLK] = first
        for n in (0, 2):
            vec_copy(it, n, a).start()
        sums = sums_of()
        second = precond_half(parts, 1)
        gsend[it, BLK:PACK] = second
        gsend[it, PACK:VEC] = sums
        for n in (1, 3, 7, 4):
            vec_copy(it, n, a).start()
        out = jnp.concatenate([first, second], axis=0)
        widen(0, out)
        return out, sums

    def gather_pass(it):
        vec_copy(it, 0, preva).wait_recv()
        vec_copy(it, 5, preva).start()
        vec_copy(it, 2, nexta).wait_recv()
        vec_copy(it, 6, nexta).start()

    def gather_near(it):
        vec_copy(it, 1, preva).wait_recv()
        widen(3, gin[it, preva, 0:PACK])
        vec_copy(it, 3, nexta).wait_recv()
        vec_copy(it, 7, nexta).wait_recv()
        widen(1, gin[it, nexta, 0:PACK])

    def gather_end(it, sums):
        for n in (4, 5, 6):
            vec_copy(it, n, oppa).wait_recv()
        widen(2, gin[it, oppa, 0:PACK])
        total = sums
        for ra in (preva, nexta, oppa):
            total = total + gin[it, ra, PACK:VEC]
        return total

    def column_sum(x, y):
        s = jnp.sum(x * y, axis=0, keepdims=True)
        return s + half_swap(s)

    row8 = iota((8, LANES), 0)

    def partial_sums(r, u, w):
        one, two = column_sum(r, u), column_sum(w, u)
        return jnp.where(row8 == 0, one, jnp.where(row8 == 1, two, 0.0))

    nothing = jnp.zeros((8, LANES), F32)
    u, _ = gather_start(0, r, lambda: nothing)
    mat_copy(5, prevc, c_right).start()
    mat_copy(7, nextc, c_left).start()
    mat_copy(1, prevc, c_left).wait_recv()
    mat_copy(8, prevc, c_left).wait_recv()
    store_rows(prevc)
    mat_copy(3, nextc, c_right).wait_recv()
    mat_copy(9, nextc, c_right).wait_recv()
    store_rows(nextc)

    gather_pass(0)
    for k in (c, prevc, nextc):
        product_rows(k, (0,))
    gather_near(0)
    for k in (c, prevc, nextc):
        product_rows(k, (1, 3))
    gather_end(0, nothing)
    for k in (c, prevc, nextc):
        product_rows(k, (2,))
    for n in range(4, 8):
        mat_copy(n, oppc, c_right).wait_recv()
    store_rows(oppc)
    product_rows(oppc, (0, 1, 3, 2))
    w = jnp.concatenate(
        [jnp.where(low_blk, by_rows[kk], by_rows[2 + kk]) for kk in range(2)], axis=0)

    gamma = alpha = None
    x = p = s = q = z = None
    for it in range(1, ITERS):
        m, sums = gather_start(it, w, lambda: partial_sums(r, u, w))
        partial[...] = product(0)
        gather_pass(it)
        gather_near(it)
        partial[...] = partial[...] + product(1) + product(3)
        total = gather_end(it, sums)
        n = partial[...] + product(2)
        gamma_new, delta = total[0:1], total[1:2]
        if it == 1:
            alpha = gamma_new / delta
            z, q, s, p = n, m, w, u
            x = alpha * p
        else:
            beta = gamma_new / gamma
            alpha = gamma_new / (delta - beta * gamma_new / alpha)
            z, q, s, p = n + beta * z, m + beta * q, w + beta * s, u + beta * p
            x = x + alpha * p
        gamma = gamma_new
        r = r - alpha * s
        u = u - alpha * q
        w = w - alpha * z

    sums = partial_sums(r, u, w)
    ssend[...] = sums
    for n, dev in ((2, a_opp), (0, a_right), (1, a_left)):
        rcopy(ssend, sin.at[n], ss, sr, dev).start()
    all_sums = rcopy(sin, sin, ss, sr, a_right)

    low_slots = low_half((SUB * HALF, LANES))

    def reply_of(v):
        vs_ = side_by_side(v)
        return jnp.where(low_slots, fold(dot(land_t[0], vs_)), fold(dot(land_t[1], vs_)))

    for n, v in ((0, x), (1, u), (2, p)):
        answers[n] = reply_of(v)
    all_sums.wait_recv()
    total = sums + sin[0] + sin[1] + sin[2]
    gamma_new, delta = total[0:1], total[1:2]
    beta = gamma_new / gamma
    alpha = gamma_new / (delta - beta * gamma_new / alpha)
    reply = answers[0] + alpha * (answers[1] + beta * answers[2])
    psend[...] = reply.reshape(SUB, HALF, LANES)
    mine = 4 * a + c

    for da, dc in far:
        peer = at(ring(a, da), ring(c, dc))
        rcopy(psend.at[peer, body], pin.at[mine], ps, pr, (owner, peer)).start()
    all_back = rcopy(pin.at[peers], pin.at[peers], ps, pr, c_right)

    pin[mine] = psend[sub, body]

    rbuf[...] = r - alpha * (w + beta * s)
    for slot, dev in ((oppc, c_opp), (nextc, c_right), (prevc, c_left)):
        source = rbuf.at[pl.ds(pl.multiple_of(lax.rem(slot, 2) * BLK, 8), BLK)]
        rcopy(source, rin.at[c], rs, rr, dev).start()
    all_resid = rcopy(rin.at[three], rin.at[three], rs, rr, c_right)
    rin[c] = rbuf[pl.ds(pl.multiple_of(lax.rem(c, 2) * BLK, 8), BLK)]

    all_back.wait_recv()

    for ra in range(4):
        for t in range(2):
            one, two = pin[4 * ra + 2 * t], pin[4 * ra + 2 * t + 1]
            cols = slice(LANES * t, LANES * (t + 1))
            back[LANES * ra:LANES * ra + MSG, cols] = jnp.where(low_msg, one, half_swap(two))
            back[LANES * ra + HALF:LANES * ra + HALF + MSG, cols] = jnp.where(
                low_msg, half_swap(one), two)
    back_hi, back_lo = split(back[...])
    mine_back = (dot(pick_t[...], back_hi) + dot(pick_t[...], back_lo)).T
    cmain[...] = mine_back[:, :LANES].reshape(OWN, 8, LANES)
    for k in range(4):
        tails = None
        for j in range(8):
            src = 8 * k + j
            piece = mine_back[8 * src:8 * (src + 1), LANES:]
            tails = piece if j == 0 else tails + pltpu.roll(piece, 16 * j, 1)
        moved = block_transpose(tails)
        for j in range(8):
            ctail[8 * k + j] = moved[j:j + 1, :]

    def send_correction(peer):
        rcopy(cmain.at[peer], cmain_in.at[owner], cs_m, cr_m, (peer, sub)).start()
        rcopy(ctail.at[peer], ctail_in.at[owner], cs_t, cr_t, (peer, sub)).start()

    each_owner(send_correction)

    c_main = rcopy(cmain.at[others], cmain_in.at[others], cs_m, cr_m, c_right)
    c_tail = rcopy(ctail.at[others], ctail_in.at[others], cs_t, cr_t, c_right)

    cmain_in[owner] = cmain[owner]
    ctail_in[owner] = ctail[owner]

    all_resid.wait_recv()
    for t in range(2):
        one, two = rin[2 * t], rin[2 * t + 1]
        upper_half = jnp.where(low_blk, half_swap(one), two)
        lower_half = jnp.where(low_blk, one, half_swap(two))
        resid_ref[:, LANES * t:LANES * (t + 1)] = jnp.where(c < 2, lower_half, upper_half)

    rcopy(rows_in.at[three], rows_in.at[three], ms, mr.at[0], c_right).wait_send()
    for it in range(ITERS):
        rcopy(gin.at[it, three], gin.at[it, three], gs.at[it], gr.at[0, 0], c_right).wait_send()
    for sent in (z_main, z_tail, all_offs, all_inv, all_vals, all_sums, all_back, all_resid):
        sent.wait_send()
    c_main.wait_recv()
    c_tail.wait_recv()
    c_main.wait_send()
    c_tail.wait_send()

    for k in range(4):
        tails = block_transpose(ctail_in[8 * k:8 * (k + 1)].reshape(8, LANES))
        turned = [
            cmain_in[8 * k + j] if j == 0 else pltpu.roll(cmain_in[8 * k + j], 16 * j, 1)
            for j in range(8)
        ]
        for m in range(9):
            if m == 0:
                value = turned[0]
            else:
                value = jnp.where(lane < 16 * m, tails, turned[m]) if m < 8 else tails
                value = jnp.where(lane < 16 * (m - 1), turned[m - 1], value)
            where_to = LANES * (9 * k + m)
            corr_ref[:, where_to:where_to + LANES] = value


def hand_on(corr_in, resid_in, corr_out, resid_out):
    corr_out[...] = corr_in[...]
    resid_out[...] = resid_in[...]


def shards(residual, counts, assembly, level_two, block_inverse):
    vmem = pl.BlockSpec(memory_space=pltpu.VMEM)
    anywhere = pl.BlockSpec(memory_space=pl.ANY)
    V = pltpu.VMEM
    dma = pltpu.SemaphoreType.DMA
    scratch = [
        pltpu.SMEM(counts.shape, jnp.int32),
        V(residual.shape, F32), V((PRIM, SIDE, SUB * BLK), jnp.int32), V((BLK, BLK), F32),
        V((BLK + TAIL, LANES), F32),
        V((OWN, 8, LANES), F32), V((OWN, 1, LANES), F32),
        V((OWN, 8, LANES), F32), V((OWN, 1, LANES), F32),
        V((OWN, 8, LANES), F32), V((OWN, 1, LANES), F32),
        V((OWN, 8, LANES), F32), V((OWN, 1, LANES), F32),
        V((SIDE, 1, LANES), F32), V((SUB, 1, LANES), F32), V((8, 256), F32),
        V((SIDE, BLK, SUB * BLK), F32), V((SIDE, BLK + TAIL, LANES), F32),
        V((SIDE, BLK, BLK), F32),
        V((SIDE, 2 * SIDE * BLK, 5 * LANES), BF16), V((SIDE, 2 * BLK, BLK), BF16),
        V((SUB, MSG, LANES), F32), V((SUB, HALF, LANES), F32),
        V((2, PACK, SUB * HALF), BF16), V((2, SUB * HALF, PACK), BF16), V((4 * LANES, 256), BF16),
        V((256, 4 * LANES), BF16),
        V((ITERS, VEC, LANES), F32), V((ITERS, SIDE, VEC, LANES), F32),
        V((SIDE, SIDE * BLK, 2 * LANES), BF16), V((8, LANES), F32), V((3, 8, LANES), F32),
        V((SUB, HALF, LANES), F32), V((SUB, MSG, LANES), F32), V((4 * LANES, 256), F32),
        V((PACK, LANES), F32), V((SIDE, BLK, LANES), F32), V((256, 256), F32), V((PACK, LANES), F32),
        V((SIDE, BLK, LANES), F32), V((3, SUB * HALF, LANES), F32),
        dma((5,)),
        dma, dma, dma, dma, dma, dma, dma, dma,
        dma, dma, dma, dma((10,)), dma, dma,
        dma, dma, dma((ITERS,)), dma((2, 8)), dma, dma,
        dma, dma, dma, dma,
    ]
    corr, resid = pl.pallas_call(
        kernel,
        out_shape=(
            jax.ShapeDtypeStruct(residual.shape, F32),
            jax.ShapeDtypeStruct((BLK, 8 * OWN), F32),
        ),
        in_specs=[anywhere] * 5,
        out_specs=(vmem, vmem),
        scratch_shapes=scratch,
        compiler_params=pltpu.CompilerParams(
            collective_id=0, has_side_effects=True, vmem_limit_bytes=62 * 1024 * 1024
        ),
    )(counts, residual, jnp.transpose(assembly[0], (1, 0, 2)), level_two[0], block_inverse[0])
    corr, resid = pl.pallas_call(
        hand_on,
        out_shape=(
            jax.ShapeDtypeStruct(corr.shape, F32), jax.ShapeDtypeStruct(resid.shape, F32)
        ),
        in_specs=[vmem, vmem],
        out_specs=(vmem, vmem),
    )(corr, resid)
    return corr, resid[None]


def solution(mesh):
    in_specs = (
        P("owner", "sub"),
        P("owner", "sub"),
        P("owner", "sub", None, None),
        P("owner", "sub", None),
        P("owner", "sub", None),
    )
    out_specs = (P("owner", "sub"), P("owner", "sub", None))
    return jax.shard_map(shards, mesh=mesh, in_specs=in_specs, out_specs=out_specs, check_vma=False)
```
